128 devices in a mesh: row: 16 (over x, z), col: 8 (over y, core).
Axes of the slice: x: 4, y: 4, z: 4, core: 2. Of those that a mesh axis runs over, the one named last changes fastest.
Arguments:
- front: float32 [9216, 9216], P('row', 'col')
- child_tiles: float32 [16384, 4096], P(('row', 'col')), may hold values from -0.4375 to 0.4375
- tile_target: int32 [16384], P(('row', 'col')), may hold values from 0 to 20735, as said below
- tile_count: int32 [512], P(('row', 'col')), may hold values from 24 to 32
- probe: float32 [9216, 512], P('col'), may hold values from -1.75 to 1.75
Outputs:
- panel_factor: float32 [9216, 1024], P('row', 'col')
- sketch: float32 [9216, 512], P('row', 'col')
The draws below stay inside these ranges and needn't reach their ends.
Inputs may be any that keep to these rules, and one draw needn't show every extreme that they name: `tile_target`: among the 128 slots of one device, live or not, each counted once at its target tile and once at the mirrored tile, at most 2 placements fall inside the block of the front held by any one device.
All inputs are finite; a program needn't handle non-finite values.
Results may differ from the reference program's by a relative error of at most 0.00015.
Values sent between devices are 32-bit elements; how exact they have to be, the bound alone decides.
A program may use at most 128 MiB of HBM per device.

```python
import math
import jax
import jax.numpy as jnp
from jax import lax

F = 9216
NB = 512
PANELS = 2
SK = 512
TB = 64
CHILDREN = 4
SLOTS = 32
CAP = 2
N_ROW = 16
N_COL = 8
DEVICES = 128


def draw_front(key, part):
    first, second, scale_key = jax.random.split(jax.random.fold_in(key, 11), 3)
    noise = jax.random.normal(first, (F, F), jnp.float32)
    symmetric = (noise + noise.T) * (3.0 / math.sqrt(2.0 * F))
    scales = jax.random.uniform(scale_key, (F,), jnp.float32, 1.2, 2.4)
    positions = jnp.arange(F, dtype=jnp.float32)
    offsets = positions[:, None] - positions[None, :]
    kernel = scales[:, None] * scales[None, :] * jnp.exp(offsets * offsets * (-0.5 / 1600.0))
    diagonal = jax.random.uniform(second, (F,), jnp.float32, 14.0, 28.0)
    spots = jnp.arange(F)
    return (symmetric + kernel).at[spots, spots].add(diagonal)


def draw_tile_target(key, part):
    base = jax.random.fold_in(key, 23)
    hot_key, source_key = jax.random.split(base)
    hot_row_key, hot_col_key = jax.random.split(hot_key)
    held = CHILDREN * SLOTS
    grid = F // TB
    tile_rows = F // N_ROW // TB
    tile_cols = F // N_COL // TB
    group = N_ROW // N_COL
    half = CAP // 2
    hot_row = jax.random.randint(hot_row_key, (), 0, N_ROW, dtype=jnp.int32)
    hot_shift = jax.random.randint(hot_col_key, (), 0, N_COL - 1, dtype=jnp.int32)
    hot_col = (hot_row // group + 1 + hot_shift) % N_COL
    hottest = hot_row * N_COL + hot_col
    pre_row = hot_col * group + hot_row % group
    pre_col = hot_row // group
    preimage = pre_row * N_COL + pre_col
    skip = (preimage - hottest - 1) % DEVICES

    def one_source(source):
        order_key, row_key, col_key = jax.random.split(source, 3)
        order = jax.random.permutation(order_key, (DEVICES - 2) * half).astype(jnp.int32) // half
        shifted = order + (order >= skip).astype(jnp.int32)
        others = (hottest + 1 + shifted) % DEVICES
        owners = jnp.concatenate([jnp.full((half,), hottest, jnp.int32), jnp.full((half,), preimage, jnp.int32), others[:held - 2 * half]])
        owner_row = owners // N_COL
        owner_col = owners % N_COL
        rows_in = jax.random.randint(row_key, (held,), 0, tile_rows, dtype=jnp.int32)
        cols_in = jax.random.randint(col_key, (held,), 0, tile_rows, dtype=jnp.int32)
        target_row = owner_row * tile_rows + rows_in
        target_col = owner_col * tile_cols + owner_row % group * tile_rows + cols_in
        return target_row * grid + target_col
    return jax.vmap(one_source)(jax.random.split(source_key, DEVICES)).reshape(-1).astype(jnp.int32)


def set_ends(values, key, least, largest):
    spot = [jax.random.randint(jax.random.fold_in(key, axis), (), 0, length) for axis, length in enumerate(values.shape)]
    main_axis = values.shape.index(max(values.shape))
    neighbour = spot[:main_axis] + [(spot[main_axis] + 1) % values.shape[main_axis]] + spot[main_axis + 1:]
    return values.at[tuple(spot)].set(least).at[tuple(neighbour)].set(largest)


def steps_of(stream_key, shape, cuts, smallest, high):
    def one(dim, blocks):
        heights = jax.random.uniform(jax.random.fold_in(jax.random.fold_in(stream_key, 6), dim), (blocks,), jnp.float32, smallest / len(cuts), high / len(cuts))
        return jnp.repeat(jnp.exp(heights), shape[dim] // blocks).reshape((-1,) + (1,) * (len(shape) - dim - 1))

    loudness = one(*cuts[0])
    for cut in cuts[1:]:
        loudness = loudness * one(*cut)
    return loudness


def gaussian(stream_key, dims, width, bound, shards=(), kind=jnp.bfloat16):
    entries = jax.random.normal(stream_key, dims, jnp.float32) * width
    if len(shards) > 0:
        entries = steps_of(stream_key, dims, shards, -0.22, 0.18) * entries
    return jnp.clip(entries, min=-bound, max=bound).astype(kind)


def setup_inputs(seed: int = 0) -> dict:
    splits = jax.random.split(jax.random.key(seed), 6)
    front = draw_front(jax.random.fold_in(splits[5], 71), 0)
    child_tiles = gaussian(splits[1], (DEVICES * CHILDREN * SLOTS, TB * TB), 0.03, 0.4375, ((0, 128),), jnp.float32)
    tile_target = draw_tile_target(jax.random.fold_in(splits[5], 71), 0)
    tile_count = set_ends(jax.random.randint(splits[3], (DEVICES * CHILDREN,), SLOTS - SLOTS // 4, SLOTS + 1), jax.random.fold_in(splits[3], 1), SLOTS - SLOTS // 4, SLOTS).astype(jnp.int32)
    probe = gaussian(splits[4], (F, SK), 0.12, 1.75, ((0, 8),), jnp.float32)
    return dict(front=front, child_tiles=child_tiles, tile_target=tile_target, tile_count=tile_count, probe=probe)


HIGH = lax.Precision.HIGHEST

def reference(front, child_tiles, tile_target, tile_count, probe):
    grid = F // TB
    index = jnp.arange(DEVICES * CHILDREN * SLOTS, dtype=jnp.int32)
    live = index % SLOTS < tile_count[index // SLOTS]
    weighted = jnp.where(live[:, None], child_tiles, jnp.zeros_like(child_tiles))
    squares = weighted.reshape(-1, TB, TB)
    tile_row = tile_target // grid
    tile_col = tile_target % grid
    blocks = jnp.zeros((grid, grid, TB, TB), front.dtype)
    blocks = blocks.at[tile_row, tile_col].add(squares)
    blocks = blocks.at[tile_col, tile_row].add(squares.transpose(0, 2, 1))
    extend = blocks.transpose(0, 2, 1, 3).reshape(F, F)
    matrix = front + extend
    factors = []
    for k in range(PANELS):
        low = k * NB
        high = low + NB
        diag_block = matrix[low:high, low:high]
        chol = jnp.linalg.cholesky(0.5 * (diag_block + diag_block.T))
        below = matrix[low:, low:high]
        solved = jax.scipy.linalg.solve_triangular(chol, below.T, lower=True).T
        factors.append(jnp.pad(solved, ((low, 0), (0, 0))))
        trail = solved[NB:]
        matrix = matrix.at[high:, high:].add(-jnp.dot(trail, trail.T, precision=HIGH))
    panel_factor = jnp.concatenate(factors, axis=1)
    start = PANELS * NB
    lower_part = jnp.dot(matrix[start:, start:], probe[start:], precision=HIGH)
    sketch = jnp.pad(lower_part, ((start, 0), (0, 0)))
    return (panel_factor, sketch)
```

```python
import functools

import jax
import jax.numpy as jnp
from jax import lax
from jax.experimental import pallas as pl
from jax.experimental.pallas import tpu as pltpu
from jax.sharding import PartitionSpec as P

NB = 512
PANELS = 2
TB = 64
SLOTS = 32
LANES = 128
SUB = 16
BLK = 128

HIGH = lax.Precision.HIGHEST
GOOD = lax.Precision.HIGH

def factor_rows(rows, base):
    sub = lax.broadcasted_iota(jnp.int32, (8, BLK), 0)
    sub2 = lax.broadcasted_iota(jnp.int32, (8, 2 * BLK), 0)
    spread = [
        [
            jnp.broadcast_to(rows[g][:, base + i : base + i + 1], (8, BLK)) if i < 8 * g + 8 else None
            for i in range(SUB)
        ]
        for g in range(2)
    ]
    rows = list(rows)
    for i in range(SUB):
        own, at = divmod(i, 8)
        pivot = jnp.broadcast_to(spread[own][i][at : at + 1, :], (8, BLK))
        scale = lax.rsqrt(pivot)
        scale2 = jnp.concatenate([scale, scale], axis=1)
        line = jnp.broadcast_to(rows[own][at : at + 1, :], (8, 2 * BLK)) * scale2
        lows = []
        for g in range(2):
            if g < own:
                lows.append(None)
                continue
            low = spread[g][i] * scale
            if g == own:
                low = jnp.where(sub > at, low, 0.0)
            lows.append(low)
        for j in range(i + 1, SUB):
            g_j, at_j = divmod(j, 8)
            factor = jnp.broadcast_to(lows[g_j][at_j : at_j + 1, :], (8, BLK))
            for g in range(g_j, 2):
                spread[g][j] = spread[g][j] - lows[g] * factor
        for g in range(own, 2):
            low2 = jnp.concatenate([lows[g], lows[g]], axis=1)
            new = rows[g] - low2 * line
            if g == own:
                new = jnp.where(sub2 == at, line, new)
            rows[g] = new
    return rows


def inverse_factor(x_ref):
    for s in range(BLK // SUB):
        base = s * SUB
        rows = factor_rows([x_ref[base : base + 8, :], x_ref[base + 8 : base + 16, :]], base)
        x_ref[base : base + 8, :] = rows[0]
        x_ref[base + 8 : base + 16, :] = rows[1]
        if base + SUB < BLK:
            done = jnp.concatenate(rows, axis=0)
            gone = lax.dot_general(
                done[:, :BLK].T, done, (((1,), (0,)), ((), ())), precision=HIGH,
                preferred_element_type=jnp.float32,
            )
            x_ref[base + SUB :, :] = x_ref[base + SUB :, :] - gone[base + SUB :, :]


def cholesky_kernel(d_ref, w_ref, a_ref, x_ref):
    n = d_ref.shape[0]
    blocks = n // BLK
    a_ref[...] = d_ref[...]
    w_ref[...] = jnp.zeros_like(w_ref)
    eye = (
        lax.broadcasted_iota(jnp.int32, (BLK, BLK), 0) == lax.broadcasted_iota(jnp.int32, (BLK, BLK), 1)
    ).astype(jnp.float32)

    def dot(a, b):
        return lax.dot_general(a, b, (((1,), (0,)), ((), ())), precision=HIGH, preferred_element_type=jnp.float32)

    for b in range(blocks):
        lo, hi = b * BLK, (b + 1) * BLK
        diag = a_ref[lo:hi, lo:hi]
        x_ref[:, :BLK] = 0.5 * (diag + diag.T)
        x_ref[:, BLK:] = eye
        inverse_factor(x_ref)
        w_diag = x_ref[:, BLK:]
        w_ref[lo:hi, lo:hi] = w_diag
        if b:
            w_ref[lo:hi, :lo] = dot(w_diag, w_ref[lo:hi, :lo])
        if b + 1 < blocks:
            upper = dot(w_diag, a_ref[lo:hi, hi:])
            a_ref[lo:hi, hi:] = upper
            for i in range(b + 1, blocks):
                low, top = i * BLK, (i + 1) * BLK
                left = a_ref[lo:hi, low:top].T
                a_ref[low:top, low:] = a_ref[low:top, low:] - dot(left, a_ref[lo:hi, low:])
                w_ref[low:top, :hi] = w_ref[low:top, :hi] - dot(left, w_ref[lo:hi, :hi])


def inverse_of_factor(d):
    n = d.shape[0]
    return pl.pallas_call(
        cholesky_kernel,
        out_shape=jax.ShapeDtypeStruct((n, n), jnp.float32),
        in_specs=[pl.BlockSpec(memory_space=pltpu.VMEM)],
        out_specs=pl.BlockSpec(memory_space=pltpu.VMEM),
        scratch_shapes=[pltpu.VMEM((n, n), jnp.float32), pltpu.VMEM((BLK, 2 * BLK), jnp.float32)],
        compiler_params=pltpu.CompilerParams(vmem_limit_bytes=48 << 20),
        cost_estimate=pl.CostEstimate(flops=2_000_000_000, bytes_accessed=8 << 20, transcendentals=0),
        name="inverse_of_factor",
    )(d)


def pack_kernel(source_ref, tiles_ref, out_ref, laid_ref, *, pitch, unroll):
    held = tiles_ref.shape[0]
    chunks = tiles_ref.shape[1] // LANES
    for group in range(held // 8):
        for part in range(chunks):
            laid_ref[pl.ds(group * 8 * pitch + part, 8, stride=pitch), :] = tiles_ref[
                group * 8 : group * 8 + 8, part * LANES : (part + 1) * LANES
            ]

    def step(q, carry):
        start = pl.multiple_of(source_ref[q] * pitch, 8)
        out_ref[q] = laid_ref[pl.ds(start, chunks), :]
        return carry

    lax.fori_loop(0, out_ref.shape[0], step, 0, unroll=unroll)


def packed(tiles, source):
    held, width = tiles.shape
    chunks = width // LANES
    pitch = chunks + 8
    return pl.pallas_call(
        functools.partial(pack_kernel, pitch=pitch, unroll=4),
        out_shape=jax.ShapeDtypeStruct((source.shape[0], chunks, LANES), jnp.float32),
        in_specs=[pl.BlockSpec(memory_space=pltpu.SMEM), pl.BlockSpec(memory_space=pltpu.VMEM)],
        out_specs=pl.BlockSpec(memory_space=pltpu.VMEM),
        scratch_shapes=[pltpu.VMEM((held * pitch, LANES), jnp.float32)],
        compiler_params=pltpu.CompilerParams(vmem_limit_bytes=32 << 20),
        cost_estimate=pl.CostEstimate(flops=10_000_000, bytes_accessed=6 << 20, transcendentals=0),
        name="packed_tiles",
    )(source, tiles)


def place_kernel(code_ref, tiles_ref, front_ref, out_ref, sum_ref, *, unroll):
    rows, cols = front_ref.shape
    blocks = cols // LANES
    flips = -(-rows // LANES)
    half_rows = TB * TB // LANES
    sum_ref[...] = jnp.zeros_like(sum_ref)
    left = lax.broadcasted_iota(jnp.int32, (half_rows, LANES), 1) < TB

    def step(q, carry):
        code = code_ref[q]
        start = pl.multiple_of((code // 2) * TB, TB)
        odd = code % 2
        tile = tiles_ref[q]
        turned = pltpu.roll(tile, TB, 1)
        is_left = odd == 0
        keep = left == is_left
        upper = jnp.where(keep, jnp.where(is_left, tile, turned), 0.0)
        lower = jnp.where(keep, jnp.where(is_left, turned, tile), 0.0)
        even = pl.ds(start, half_rows, stride=2)
        uneven = pl.ds(start + 1, half_rows, stride=2)
        sum_ref[even, :] = sum_ref[even, :] + upper
        sum_ref[uneven, :] = sum_ref[uneven, :] + lower
        return carry

    lax.fori_loop(0, tiles_ref.shape[0], step, 0, unroll=unroll)
    for block in range(blocks):
        lo, hi = block * LANES, (block + 1) * LANES
        out_ref[:, lo:hi] = front_ref[:, lo:hi] + sum_ref[block * rows : (block + 1) * rows, :]
        for flip in range(flips):
            at = blocks * rows + flip * cols + lo
            size = min(LANES, rows - flip * LANES)
            span = slice(flip * LANES, flip * LANES + size)
            out_ref[span, lo:hi] = out_ref[span, lo:hi] + sum_ref[at : at + LANES, :].T[:size, :]


def placed(front, tiles, code):
    rows, cols = front.shape
    total = (cols // LANES) * rows + -(-rows // LANES) * cols + TB
    return pl.pallas_call(
        functools.partial(place_kernel, unroll=8),
        out_shape=jax.ShapeDtypeStruct(front.shape, jnp.float32),
        in_specs=[pl.BlockSpec(memory_space=pltpu.SMEM)] + [pl.BlockSpec(memory_space=pltpu.VMEM)] * 2,
        out_specs=pl.BlockSpec(memory_space=pltpu.VMEM),
        scratch_shapes=[pltpu.VMEM((total, LANES), jnp.float32)],
        compiler_params=pltpu.CompilerParams(vmem_limit_bytes=32 << 20),
        cost_estimate=pl.CostEstimate(flops=10_000_000, bytes_accessed=10 << 20, transcendentals=0),
        name="placed_tiles",
    )(code, tiles, front)


MESH = pl.DeviceIdType.MESH


def share_kernel(
    matrix_ref, z_ref, y_ref, d_ref, z_all_ref, y_own_ref,
    z_in, y_in, first_send, next_send, d_recv, z_send, z_recv, zall_send, zall_recv, y_send, y_recv,
):
    me_row, me_col = lax.axis_index("row"), lax.axis_index("col")
    n_row, n_col = z_in.shape[0], y_in.shape[0]
    order = d_ref.shape[0]
    local_rows = matrix_ref.shape[0]
    piece = order // n_row
    z_lines, y_lines = z_in.shape[1], y_in.shape[1]

    def y_copy(step):
        to = lax.rem(me_col + step, n_col)
        return pltpu.make_async_remote_copy(
            y_ref.at[pl.ds(pl.multiple_of(to * y_lines, 8), y_lines)], y_in.at[me_col],
            y_send.at[to], y_recv.at[me_col], device_id=(me_row, to), device_id_type=MESH,
        )

    def z_copy(step):
        to = lax.rem(me_row + step, n_row)
        return pltpu.make_async_remote_copy(
            z_ref.at[pl.ds(pl.multiple_of(to * z_lines, 8), z_lines)], z_in.at[me_row],
            z_send.at[to], z_recv.at[me_row], device_id=(to, me_col), device_id_type=MESH,
        )

    def z_all_copy(step):
        to = lax.rem(me_row + step, n_row)
        mine = z_all_ref.at[pl.ds(pl.multiple_of(me_row * z_lines, 8), z_lines)]
        return pltpu.make_async_remote_copy(
            mine, mine, zall_send.at[to], zall_recv.at[me_row], device_id=(to, me_col), device_id_type=MESH,
        )

    def cut(j):
        return j * piece // 128 * 128

    def d_piece(j):
        return d_ref.at[j * piece : (j + 1) * piece, cut(j) : order]

    def arrived(into, sem):
        pltpu.make_async_copy(into, into, sem).wait()

    def first_copy(j):
        at = j * piece % local_rows
        return pltpu.make_async_remote_copy(
            matrix_ref.at[at : at + piece, cut(j) : order],
            d_piece(j),
            first_send.at[j], d_recv.at[j], device_id=(j, me_col), device_id_type=MESH,
        )

    def next_copy(j, step):
        to = lax.rem(j + step, n_row)
        here = d_piece(j)
        source = matrix_ref.at[0:piece, 0:order] if j == 0 else here
        return pltpu.make_async_remote_copy(
            source, here, next_send.at[to], d_recv.at[j], device_id=(to, me_col), device_id_type=MESH,
        )

    def each(count, action):
        def step(s, carry):
            action(s)
            return carry
        lax.fori_loop(1, count, step, 0)

    for root in range(2):
        @pl.when((me_col == 0) & (me_row == root))
        def _():
            for j in range(max(1, root * local_rows // piece), min(n_row, (root + 1) * local_rows // piece)):
                first_copy(j).start()
            if root == 0:
                d_ref[0:piece, :] = matrix_ref[0:piece, 0:order]
                each(n_row, lambda s: next_copy(0, s).start())

    @pl.when(me_col == 0)
    def _():
        each(n_row, lambda s: z_copy(s).start())

    each(n_col, lambda s: y_copy(s).start())

    for j in range(1, n_row):
        @pl.when((me_col == 0) & (me_row == j))
        def _():
            arrived(d_piece(j), d_recv.at[j])
            each(n_row, lambda s: next_copy(j, s).start())

    @pl.when(me_col == 0)
    def _():
        own = pl.ds(pl.multiple_of(me_row * z_lines, 8), z_lines)
        z_in[me_row] = z_ref[own, :]
        each(n_row, lambda s: arrived(z_in.at[lax.rem(me_row + s, n_row)], z_recv.at[lax.rem(me_row + s, n_row)]))
        total = z_in[0]
        for k in range(1, n_row):
            total = total + z_in[k]
        z_all_ref[own, :] = total

    each(n_col, lambda s: arrived(y_in.at[lax.rem(me_col + s, n_col)], y_recv.at[lax.rem(me_col + s, n_col)]))
    y_in[me_col] = y_ref[pl.ds(pl.multiple_of(me_col * y_lines, 8), y_lines), :]
    y_total = y_in[0]
    for k in range(1, n_col):
        y_total = y_total + y_in[k]
    y_own_ref[...] = y_total

    @pl.when(me_col == 0)
    def _():
        each(n_row, lambda s: z_all_copy(s).start())
        for j in range(n_row):
            @pl.when(me_row != j)
            def _():
                arrived(d_piece(j), d_recv.at[j])
                arrived(z_all_ref.at[j * z_lines : (j + 1) * z_lines], zall_recv.at[j])

        each(n_row, lambda s: z_copy(s).wait_send())
        each(n_row, lambda s: z_all_copy(s).wait_send())

    each(n_col, lambda s: y_copy(s).wait_send())
    for root in range(2):
        @pl.when((me_col == 0) & (me_row == root))
        def _():
            for j in range(max(1, root * local_rows // piece), min(n_row, (root + 1) * local_rows // piece)):
                first_copy(j).wait_send()
    for j in range(n_row):
        @pl.when((me_col == 0) & (me_row == j))
        def _():
            each(n_row, lambda s: next_copy(j, s).wait_send())


def shared(matrix, z_part, y_part, order, n_row, n_col):
    lines_z, lines_y = z_part.shape[0] // n_row, y_part.shape[0] // n_col
    dma = pltpu.SemaphoreType.DMA
    return pl.pallas_call(
        share_kernel,
        out_shape=(
            jax.ShapeDtypeStruct((order, order), jnp.float32),
            jax.ShapeDtypeStruct(z_part.shape, jnp.float32),
            jax.ShapeDtypeStruct((lines_y, y_part.shape[1]), jnp.float32),
        ),
        in_specs=[pl.BlockSpec(memory_space=pltpu.VMEM)] * 3,
        out_specs=[pl.BlockSpec(memory_space=pltpu.VMEM)] * 3,
        scratch_shapes=[
            pltpu.VMEM((n_row, lines_z, z_part.shape[1]), jnp.float32),
            pltpu.VMEM((n_col, lines_y, y_part.shape[1]), jnp.float32),
            *[dma((n_row,))] * 7,
            *[dma((n_col,))] * 2,
        ],
        compiler_params=pltpu.CompilerParams(has_side_effects=True, vmem_limit_bytes=40 << 20),
        cost_estimate=pl.CostEstimate(flops=1_000_000_000, bytes_accessed=12 << 20, transcendentals=0),
        name="shared_parts",
    )(matrix, z_part, y_part)


def hand_out_kernel(solved_ref, fix_ref, panel_ref, share_ref, solved_send, solved_recv, fix_send, fix_recv):
    me_row, me_col = lax.axis_index("row"), lax.axis_index("col")
    n_col = solved_ref.shape[0]
    lines = share_ref.shape[0]

    def copies(to):
        return (
            pltpu.make_async_remote_copy(
                solved_ref.at[to], panel_ref, solved_send.at[to], solved_recv.at[0],
                device_id=(me_row, to), device_id_type=MESH,
            ),
            pltpu.make_async_remote_copy(
                fix_ref.at[pl.ds(pl.multiple_of(to * lines, 8), lines)], share_ref,
                fix_send.at[to], fix_recv.at[0], device_id=(me_row, to), device_id_type=MESH,
            ),
        )

    def each(action):
        def step(to, carry):
            action(to)
            return carry
        lax.fori_loop(1, n_col, step, 0)

    def begin(to):
        for copy in copies(to):
            copy.start()

    def finish(to):
        for copy in copies(to):
            copy.wait_send()

    @pl.when(me_col == 0)
    def _():
        each(begin)
        panel_ref[...] = solved_ref[0]
        share_ref[...] = fix_ref[0:lines, :]
        each(finish)

    @pl.when(me_col != 0)
    def _():
        pltpu.make_async_copy(panel_ref, panel_ref, solved_recv.at[0]).wait()
        pltpu.make_async_copy(share_ref, share_ref, fix_recv.at[0]).wait()


def handed_out(solved, fix):
    n_col, rows, width = solved.shape
    dma = pltpu.SemaphoreType.DMA
    return pl.pallas_call(
        hand_out_kernel,
        out_shape=(
            jax.ShapeDtypeStruct((rows, width), jnp.float32),
            jax.ShapeDtypeStruct((fix.shape[0] // n_col, fix.shape[1]), jnp.float32),
        ),
        in_specs=[pl.BlockSpec(memory_space=pltpu.VMEM)] * 2,
        out_specs=[pl.BlockSpec(memory_space=pltpu.VMEM)] * 2,
        scratch_shapes=[dma((n_col,)), dma((1,)), dma((n_col,)), dma((1,))],
        compiler_params=pltpu.CompilerParams(has_side_effects=True, vmem_limit_bytes=24 << 20),
        cost_estimate=pl.CostEstimate(flops=1_000_000_000, bytes_accessed=8 << 20, transcendentals=0),
        name="handed_out",
    )(solved, fix)


def per_device(front, child_tiles, tile_target, tile_count, probe):
    n_row, n_col = lax.axis_size("row"), lax.axis_size("col")
    devices = n_row * n_col
    me_row, me_col = lax.axis_index("row"), lax.axis_index("col")
    rows, cols = front.shape
    tile_rows, tile_cols = rows // TB, cols // TB
    grid = tile_cols * n_col
    held = child_tiles.shape[0]
    start = PANELS * NB
    slot_index = jnp.arange(held, dtype=jnp.int32)
    live = slot_index % SLOTS < tile_count[slot_index // SLOTS]
    first_row, first_col = tile_target // grid, tile_target % grid
    target_row = jnp.concatenate([first_row, first_col])
    target_col = jnp.concatenate([first_col, first_row])
    owner = target_row // tile_rows * n_col + target_col // tile_cols
    in_row, in_col = target_row % tile_rows, target_col % tile_cols
    upright = jnp.arange(2 * held) < held
    upright_code = 2 * (in_col // 2 * tile_rows + in_row) + in_col % 2
    blocks = cols // LANES * tile_rows
    flips = -(-rows // LANES) * tile_cols
    turned_code = 2 * (blocks + in_row // 2 * tile_cols + in_col) + in_row % 2
    code = jnp.where(upright, upright_code, turned_code)
    code = jnp.where(jnp.concatenate([live, live]), code, 2 * (blocks + flips))
    order = jnp.arange(2 * held, dtype=jnp.int32)
    same = (owner[:, None] == owner[None, :]) & (order[None, :] < order[:, None])
    slot = 2 * owner + jnp.sum(same.astype(jnp.int32), axis=1)
    at_slot = slot[None, :] == order[:, None]
    source = jnp.sum(jnp.where(at_slot, (order % held)[None, :], 0), axis=1)
    sent_code = jnp.sum(jnp.where(at_slot, code[None, :], 0), axis=1)
    outgoing = packed(child_tiles, source)
    chunks = outgoing.shape[1]
    incoming = lax.all_to_all(
        outgoing.reshape(devices, 2, chunks, LANES), ("row", "col"), split_axis=0, concat_axis=0, tiled=True
    )
    landing = lax.all_to_all(
        sent_code.reshape(devices, 2), ("row", "col"), split_axis=0, concat_axis=0, tiled=True
    )
    group = n_row // n_col
    half = lax.dynamic_slice_in_dim(probe, me_row % group * rows, rows, 0)
    probe_rows = lax.ppermute(
        half, ("row", "col"), [(r * n_col + r // group, r * n_col) for r in range(n_row)]
    )
    matrix = placed(front, incoming.reshape(2 * devices, chunks, LANES), landing.reshape(-1))

    global_rows = me_row * rows + jnp.arange(rows, dtype=jnp.int32)
    global_cols = me_col * cols + jnp.arange(cols, dtype=jnp.int32)
    by_cols = jnp.where((global_cols >= start)[:, None], probe, 0.0)
    by_rows = jnp.where((global_rows >= start)[:, None], probe_rows, 0.0)
    y_part = lax.dot_general(by_cols, matrix, (((0,), (1,)), ((), ())), precision=GOOD)
    panel = matrix[:, :start]
    z_part = lax.dot_general(by_rows, panel, (((0,), (0,)), ((), ())), precision=GOOD)
    leading, z_all, y_own = shared(matrix, z_part, y_part, start, n_row, n_col)
    inverse = inverse_of_factor(leading)
    solved = lax.dot_general(panel, inverse, (((1,), (1,)), ((), ())), precision=GOOD)
    panel_of = jnp.arange(start, dtype=jnp.int32) // NB * NB
    solved = jnp.where(global_rows[:, None] >= panel_of[None, :], solved, 0.0)
    weights = lax.dot_general(z_all, inverse, (((1,), (1,)), ((), ())), precision=GOOD)
    fix = lax.dot_general(weights, solved, (((1,), (1,)), ((), ())), precision=GOOD)
    by_owner = solved.reshape(rows, n_col, start // n_col).transpose(1, 0, 2)
    panel_factor, fix_own = handed_out(by_owner, fix)
    sketch = jnp.where((global_rows >= start)[:, None], (y_own - fix_own).T, 0.0)
    return (panel_factor, sketch)


def solution(mesh):
    return jax.shard_map(
        per_device,
        mesh=mesh,
        in_specs=(
            P("row", "col"),
            P(("row", "col"), None),
            P(("row", "col")),
            P(("row", "col")),
            P("col", None),
        ),
        out_specs=(P("row", "col"), P("row", "col")),
        check_vma=False,
    )
```

```python
import functools

import jax
import jax.numpy as jnp
from jax import lax
from jax.experimental import pallas as pl
from jax.experimental.pallas import tpu as pltpu
from jax.sharding import PartitionSpec as P

NB = 512
PANELS = 2
TB = 64
SLOTS = 32
LANES = 128
SUB = 16
BLK = 128

HIGH = lax.Precision.HIGHEST
GOOD = lax.Precision.HIGH


def pack_kernel(source_ref, tiles_ref, out_ref, laid_ref, *, pitch, unroll):
    held = tiles_ref.shape[0]
    chunks = tiles_ref.shape[1] // LANES
    for group in range(held // 8):
        for part in range(chunks):
            laid_ref[pl.ds(group * 8 * pitch + part, 8, stride=pitch), :] = tiles_ref[
                group * 8 : group * 8 + 8, part * LANES : (part + 1) * LANES
            ]

    def step(q, carry):
        start = pl.multiple_of(source_ref[q] * pitch, 8)
        out_ref[q] = laid_ref[pl.ds(start, chunks), :]
        return carry

    lax.fori_loop(0, out_ref.shape[0], step, 0, unroll=unroll)


def packed(tiles, source):
    held, width = tiles.shape
    chunks = width // LANES
    pitch = chunks + 8
    return pl.pallas_call(
        functools.partial(pack_kernel, pitch=pitch, unroll=4),
        out_shape=jax.ShapeDtypeStruct((source.shape[0], chunks, LANES), jnp.float32),
        in_specs=[pl.BlockSpec(memory_space=pltpu.SMEM), pl.BlockSpec(memory_space=pltpu.VMEM)],
        out_specs=pl.BlockSpec(memory_space=pltpu.VMEM),
        scratch_shapes=[pltpu.VMEM((held * pitch, LANES), jnp.float32)],
        compiler_params=pltpu.CompilerParams(vmem_limit_bytes=32 << 20),
        cost_estimate=pl.CostEstimate(flops=10_000_000, bytes_accessed=6 << 20, transcendentals=0),
        name="packed_tiles",
    )(source, tiles)


def place_kernel(code_ref, tiles_ref, front_ref, out_ref, sum_ref, *, unroll):
    rows, cols = front_ref.shape
    blocks = cols // LANES
    flips = -(-rows // LANES)
    half_rows = TB * TB // LANES
    sum_ref[...] = jnp.zeros_like(sum_ref)
    left = lax.broadcasted_iota(jnp.int32, (half_rows, LANES), 1) < TB

    def step(q, carry):
        code = code_ref[q]
        start = pl.multiple_of((code // 2) * TB, TB)
        odd = code % 2
        tile = tiles_ref[q]
        turned = pltpu.roll(tile, TB, 1)
        is_left = odd == 0
        keep = left == is_left
        upper = jnp.where(keep, jnp.where(is_left, tile, turned), 0.0)
        lower = jnp.where(keep, jnp.where(is_left, turned, tile), 0.0)
        even = pl.ds(start, half_rows, stride=2)
        uneven = pl.ds(start + 1, half_rows, stride=2)
        sum_ref[even, :] = sum_ref[even, :] + upper
        sum_ref[uneven, :] = sum_ref[uneven, :] + lower
        return carry

    lax.fori_loop(0, tiles_ref.shape[0], step, 0, unroll=unroll)
    for block in range(blocks):
        lo, hi = block * LANES, (block + 1) * LANES
        out_ref[:, lo:hi] = front_ref[:, lo:hi] + sum_ref[block * rows : (block + 1) * rows, :]
        for flip in range(flips):
            at = blocks * rows + flip * cols + lo
            size = min(LANES, rows - flip * LANES)
            span = slice(flip * LANES, flip * LANES + size)
            out_ref[span, lo:hi] = out_ref[span, lo:hi] + sum_ref[at : at + LANES, :].T[:size, :]


def placed(front, tiles, code):
    rows, cols = front.shape
    total = (cols // LANES) * rows + -(-rows // LANES) * cols + TB
    return pl.pallas_call(
        functools.partial(place_kernel, unroll=8),
        out_shape=jax.ShapeDtypeStruct(front.shape, jnp.float32),
        in_specs=[pl.BlockSpec(memory_space=pltpu.SMEM)] + [pl.BlockSpec(memory_space=pltpu.VMEM)] * 2,
        out_specs=pl.BlockSpec(memory_space=pltpu.VMEM),
        scratch_shapes=[pltpu.VMEM((total, LANES), jnp.float32)],
        compiler_params=pltpu.CompilerParams(vmem_limit_bytes=32 << 20),
        cost_estimate=pl.CostEstimate(flops=10_000_000, bytes_accessed=10 << 20, transcendentals=0),
        name="placed_tiles",
    )(code, tiles, front)


MESH = pl.DeviceIdType.MESH


def exchange_kernel(
    tiles_ref, code_ref, probe_ref, tiles_in, code_in, probe_rows,
    tiles_send, tiles_recv, code_send, code_recv, probe_send, probe_recv,
):
    n_row, n_col = lax.axis_size("row"), lax.axis_size("col")
    devices = n_row * n_col
    me_row, me_col = lax.axis_index("row"), lax.axis_index("col")
    me = me_row * n_col + me_col
    rows = probe_rows.shape[0]
    group = n_row // n_col
    at = pl.ds(pl.multiple_of(lax.rem(me_row, group) * rows, 8), rows)

    def copies(step):
        to = lax.rem(me + step, devices)
        where_to = (to // n_col, lax.rem(to, n_col))
        return (
            pltpu.make_async_remote_copy(
                code_ref.at[to], code_in.at[me], code_send, code_recv,
                device_id=where_to, device_id_type=MESH,
            ),
            pltpu.make_async_remote_copy(
                tiles_ref.at[to], tiles_in.at[me], tiles_send, tiles_recv,
                device_id=where_to, device_id_type=MESH,
            ),
        )

    def begin(step, carry):
        for copy in copies(step):
            copy.start()
        return carry

    probe_copy = pltpu.make_async_remote_copy(
        probe_ref.at[at], probe_rows, probe_send, probe_recv, device_id=(me_row, 0), device_id_type=MESH
    )
    source_col = me_row // group
    sends_probe = (me_col == source_col) & (me_col != 0)
    gets_probe = (me_col == 0) & (source_col != 0)

    lax.fori_loop(1, devices, begin, 0)

    @pl.when(sends_probe)
    def _():
        probe_copy.start()

    @pl.when((me_col == 0) & (source_col == 0))
    def _():
        probe_rows[...] = probe_ref[at, :]

    tiles_in[me] = tiles_ref[me]
    code_in[me] = code_ref[me]
    others = pl.ds(0, devices - 1)

    def all_of(ref, sem):
        pltpu.make_async_copy(ref.at[others], ref.at[others], sem).wait()

    all_of(code_in, code_recv)
    all_of(tiles_in, tiles_recv)
    all_of(code_ref, code_send)
    all_of(tiles_ref, tiles_send)

    @pl.when(gets_probe)
    def _():
        pltpu.make_async_copy(probe_rows, probe_rows, probe_recv).wait()

    @pl.when(sends_probe)
    def _():
        probe_copy.wait_send()


def exchanged(tiles, code, probe, rows):
    dma = pltpu.SemaphoreType.DMA
    return pl.pallas_call(
        exchange_kernel,
        out_shape=(
            jax.ShapeDtypeStruct(tiles.shape, jnp.float32),
            jax.ShapeDtypeStruct(code.shape, jnp.int32),
            jax.ShapeDtypeStruct((rows, probe.shape[1]), jnp.float32),
        ),
        in_specs=[pl.BlockSpec(memory_space=pltpu.VMEM)] * 3,
        out_specs=[pl.BlockSpec(memory_space=pltpu.VMEM)] * 3,
        scratch_shapes=[dma] * 6,
        compiler_params=pltpu.CompilerParams(has_side_effects=True, vmem_limit_bytes=32 << 20),
        cost_estimate=pl.CostEstimate(flops=1_000_000_000, bytes_accessed=16 << 20, transcendentals=0),
        name="exchanged_tiles",
    )(tiles, code, probe)


def factor_rows(rows, base):
    sub = lax.broadcasted_iota(jnp.int32, (8, BLK), 0)
    lane = lax.broadcasted_iota(jnp.int32, (8, BLK), 1)

    def column(g, i):
        here = jnp.where(lane == base + i, rows[g][:, :BLK], 0.0)
        return jnp.broadcast_to(jnp.sum(here, axis=1, keepdims=True), (8, BLK))

    spread = [[column(g, i) if i < 8 * g + 8 else None for i in range(SUB)] for g in range(2)]
    halves = [[row[:, :BLK], row[:, BLK:]] for row in rows]
    for i in range(SUB):
        own, at = divmod(i, 8)
        pivot = jnp.broadcast_to(spread[own][i][at : at + 1, :], (8, BLK))
        scale = lax.rsqrt(pivot)
        lows = [None, None]
        for g in range(own, 2):
            low = spread[g][i] * scale
            lows[g] = jnp.where(sub > at, low, 0.0) if g == own else low
        for j in range(i + 1, SUB):
            g_j, at_j = divmod(j, 8)
            factor = jnp.broadcast_to(lows[g_j][at_j : at_j + 1, :], (8, BLK))
            for g in range(g_j, 2):
                spread[g][j] = spread[g][j] - lows[g] * factor
        for h in range(2):
            line = jnp.broadcast_to(halves[own][h][at : at + 1, :], (8, BLK)) * scale
            for g in range(own, 2):
                new = halves[g][h] - lows[g] * line
                halves[g][h] = jnp.where(sub == at, line, new) if g == own else new
    return [jnp.concatenate(half, axis=1) for half in halves]


def inverse_factor(x_ref, beside):
    row = lax.broadcasted_iota(jnp.int32, (BLK, 2 * BLK), 0)

    def step(s, carry):
        base = pl.multiple_of(s * SUB, SUB)
        rows = factor_rows([x_ref[pl.ds(base, 8), :], x_ref[pl.ds(base + 8, 8), :]], base)
        beside(s)
        x_ref[pl.ds(base, 8), :] = rows[0]
        x_ref[pl.ds(base + 8, 8), :] = rows[1]
        done = jnp.concatenate(rows, axis=0)
        gone = plain_dot(done[:, :BLK].T, done)
        x_ref[...] = x_ref[...] - jnp.where(row >= base + SUB, gone, 0.0)
        return carry

    lax.fori_loop(0, BLK // SUB, step, 0)


def plain_dot(a, b):
    return lax.dot_general(
        a, b, (((1,), (0,)), ((), ())), precision=HIGH, preferred_element_type=jnp.float32
    )


def halves_of(a):
    top = a.astype(jnp.bfloat16)
    return top, (a - top.astype(jnp.float32)).astype(jnp.bfloat16)


def turned_dot(a, b):
    a_top, a_rest = halves_of(a)
    b_top, b_rest = halves_of(b)

    def part(p, q):
        return lax.dot_general(p, q, (((1,), (1,)), ((), ())), preferred_element_type=jnp.float32)

    return part(a_top, b_top) + (part(a_top, b_rest) + part(a_rest, b_top))


def panel_kernel(
    matrix_ref, z_ref, y_ref, w_ref, solved_ref, panel_ref, z_all_ref, y_own_ref,
    m_ref, stage_ref, x_ref, z_in, y_in,
    first_send, first_recv, next_send, d_recv, z_send, z_recv, zall_send, zall_recv,
    y_send, y_recv, s_send, s_recv,
):
    me_row, me_col = lax.axis_index("row"), lax.axis_index("col")
    n_row, n_col = z_in.shape[0], y_in.shape[0]
    blocks, _, order = m_ref.shape
    rows = matrix_ref.shape[0]
    piece = order // n_row
    per_block = BLK // piece
    z_lines, y_lines = z_in.shape[1], y_in.shape[1]
    on_panel = me_col == 0

    def y_copy(step):
        to = lax.rem(me_col + step, n_col)
        return pltpu.make_async_remote_copy(
            y_ref.at[pl.ds(pl.multiple_of(to * y_lines, 8), y_lines)], y_in.at[me_col],
            y_send.at[to], y_recv.at[me_col], device_id=(me_row, to), device_id_type=MESH,
        )

    def z_copy(step):
        to = lax.rem(me_row + step, n_row)
        return pltpu.make_async_remote_copy(
            z_ref.at[pl.ds(pl.multiple_of(to * z_lines, 8), z_lines)], z_in.at[me_row],
            z_send.at[to], z_recv.at[me_row], device_id=(to, me_col), device_id_type=MESH,
        )

    def z_all_copy(step):
        to = lax.rem(me_row + step, n_row)
        mine = z_all_ref.at[pl.ds(pl.multiple_of(me_row * z_lines, 8), z_lines)]
        return pltpu.make_async_remote_copy(
            mine, mine, zall_send.at[to], zall_recv.at[me_row], device_id=(to, me_col), device_id_type=MESH,
        )

    def solved_copy(i):
        return pltpu.make_async_remote_copy(
            solved_ref.at[i], panel_ref, s_send.at[i], s_recv.at[0],
            device_id=(me_row, i), device_id_type=MESH,
        )

    def cut(j):
        return j // per_block * BLK

    def d_piece(j):
        at = j % per_block * piece
        return m_ref.at[j // per_block, at : at + piece, cut(j) : order]

    def from_root(j):
        at = j * piece % rows
        return matrix_ref.at[at : at + piece, cut(j) : order]

    def arrived(into, sem):
        pltpu.make_async_copy(into, into, sem).wait()

    def first_copy(j):
        return pltpu.make_async_remote_copy(
            from_root(j), stage_ref.at[:, cut(j) : order],
            first_send.at[j], first_recv.at[0], device_id=(j, me_col), device_id_type=MESH,
        )

    def next_copy(j, step):
        to = lax.rem(j + step, n_row)
        source = stage_ref.at[:, cut(j) : order] if j else from_root(0)
        return pltpu.make_async_remote_copy(
            source, d_piece(j), next_send.at[to], d_recv.at[j], device_id=(to, me_col), device_id_type=MESH,
        )

    def each(count, action):
        def step(s, carry):
            action(s)
            return carry

        lax.fori_loop(1, count, step, 0)

    roots = [
        [j for j in range(1, n_row) if j * piece // rows == root] for root in range(-(-order // rows))
    ]
    for root, pieces in enumerate(roots):
        @pl.when(on_panel & (me_row == root))
        def _(pieces=pieces):
            for j in pieces:
                first_copy(j).start()

    for j in range(n_row):
        @pl.when(on_panel & (me_row == j))
        def _(j=j):
            at = j % per_block * piece
            if j:
                arrived(stage_ref.at[:, cut(j) : order], first_recv.at[0])
                each(n_row, lambda s: next_copy(j, s).start())
                m_ref[j // per_block, at : at + piece, cut(j) : order] = stage_ref[:, cut(j) : order]
            else:
                each(n_row, lambda s: next_copy(j, s).start())
                m_ref[0, 0:piece, :] = matrix_ref[0:piece, 0:order]

    @pl.when(on_panel)
    def _():
        each(n_row, lambda s: z_copy(s).start())

    each(n_col, lambda s: y_copy(s).start())

    def sum_z():
        own = pl.ds(pl.multiple_of(me_row * z_lines, 8), z_lines)
        z_in[me_row] = z_ref[own, :]

        def wait_z(s):
            k = lax.rem(me_row + s, n_row)
            arrived(z_in.at[k], z_recv.at[k])

        each(n_row, wait_z)
        total = z_in[0]
        for k in range(1, n_row):
            total = total + z_in[k]
        z_all_ref[own, :] = total

    def sum_y():
        def wait_y(s):
            k = lax.rem(me_col + s, n_col)
            arrived(y_in.at[k], y_recv.at[k])

        each(n_col, wait_y)
        y_in[me_col] = y_ref[pl.ds(pl.multiple_of(me_col * y_lines, 8), y_lines), :]
        y_total = y_in[0]
        for k in range(1, n_col):
            y_total = y_total + y_in[k]
        y_own_ref[...] = y_total

    eye = (
        lax.broadcasted_iota(jnp.int32, (BLK, BLK), 0) == lax.broadcasted_iota(jnp.int32, (BLK, BLK), 1)
    ).astype(jnp.float32)
    slab = rows // (BLK // SUB)

    def solve_slab(i, s):
        lines = pl.ds(pl.multiple_of(s * slab, 8), slab)
        hi = (i + 1) * BLK
        part = turned_dot(matrix_ref[lines, :hi], w_ref[i, :, :hi])
        if i * BLK >= NB:
            line = me_row * rows + s * slab + lax.broadcasted_iota(jnp.int32, (slab, BLK), 0)
            part = jnp.where(line >= i * BLK // NB * NB, part, 0.0)
        solved_ref[i, lines, :] = part

    @pl.when(on_panel)
    def _():
        for i in range(blocks):
            lo, hi = i * BLK, (i + 1) * BLK
            for j in range(i * per_block, (i + 1) * per_block):
                @pl.when(me_row != j)
                def _(j=j):
                    arrived(d_piece(j), d_recv.at[j])
            own_row = m_ref[i, :, lo:]
            if i:
                left = jnp.concatenate([m_ref[b, :, lo:hi].T for b in range(i)], axis=1)
                own_row = own_row - plain_dot(left, m_ref[:i, :, lo:].reshape(lo, order - lo))
                w_ref[i, :, :lo] = -plain_dot(left, w_ref[:i, :, :lo].reshape(lo, lo))
            diag = own_row[:, :BLK]
            x_ref[:, :BLK] = 0.5 * (diag + diag.T)
            x_ref[:, BLK:] = eye
            if hi < order:
                m_ref[i, :, hi:] = own_row[:, BLK:]
            inverse_factor(x_ref, (lambda s: solve_slab(i - 1, s)) if i else (lambda s: None))
            if i > 1:
                solved_copy(i - 1).start()
            if i == 3:
                sum_z()
            w_diag = x_ref[:, BLK:]
            w_ref[i, :, lo:hi] = w_diag
            if i:
                w_ref[i, :, :lo] = plain_dot(w_diag, w_ref[i, :, :lo])
            if hi < order:
                m_ref[i, :, hi:] = plain_dot(w_diag, m_ref[i, :, hi:])
                w_ref[i, :, hi:] = jnp.zeros((BLK, order - hi), jnp.float32)
            if i == 4:
                each(n_row, lambda s: z_all_copy(s).start())

        def last(s, carry):
            solve_slab(blocks - 1, s)
            return carry

        lax.fori_loop(0, BLK // SUB, last, 0)

    sum_y()

    @pl.when(on_panel)
    def _():
        solved_copy(blocks - 1).start()
        panel_ref[...] = solved_ref[0]

        def wait_all(s):
            k = lax.rem(me_row + s, n_row)
            lines = z_all_ref.at[pl.ds(pl.multiple_of(k * z_lines, 8), z_lines)]
            arrived(lines, zall_recv.at[k])

        each(n_row, wait_all)
        each(n_row, lambda s: z_copy(s).wait_send())
        each(n_row, lambda s: z_all_copy(s).wait_send())
        each(n_col, lambda s: solved_copy(s).wait_send())

    @pl.when(me_col != 0)
    def _():
        arrived(panel_ref, s_recv.at[0])

    each(n_col, lambda s: y_copy(s).wait_send())
    for root, pieces in enumerate(roots):
        @pl.when(on_panel & (me_row == root))
        def _(pieces=pieces):
            for j in pieces:
                first_copy(j).wait_send()
    for j in range(n_row):
        @pl.when(on_panel & (me_row == j))
        def _(j=j):
            each(n_row, lambda s: next_copy(j, s).wait_send())


def panel_parts(matrix, z_part, y_part, order, n_row, n_col):
    lines_z, lines_y = z_part.shape[0] // n_row, y_part.shape[0] // n_col
    rows = matrix.shape[0]
    width = order // n_col
    dma = pltpu.SemaphoreType.DMA
    whole = functools.partial(jax.ShapeDtypeStruct, dtype=jnp.float32)
    return pl.pallas_call(
        panel_kernel,
        out_shape=(
            whole((order // BLK, BLK, order)),
            whole((n_col, rows, width)),
            whole((rows, width)),
            whole(z_part.shape),
            whole((lines_y, y_part.shape[1])),
        ),
        in_specs=[pl.BlockSpec(memory_space=pltpu.VMEM)] * 3,
        out_specs=[pl.BlockSpec(memory_space=pltpu.VMEM)] * 5,
        scratch_shapes=[
            pltpu.VMEM((order // BLK, BLK, order), jnp.float32),
            pltpu.VMEM((order // n_row, order), jnp.float32),
            pltpu.VMEM((BLK, 2 * BLK), jnp.float32),
            pltpu.VMEM((n_row, lines_z, z_part.shape[1]), jnp.float32),
            pltpu.VMEM((n_col, lines_y, y_part.shape[1]), jnp.float32),
            dma((n_row,)), dma((1,)), *[dma((n_row,))] * 6, *[dma((n_col,))] * 2, dma((n_col,)), dma((1,)),
        ],
        compiler_params=pltpu.CompilerParams(has_side_effects=True, vmem_limit_bytes=60 << 20),
        cost_estimate=pl.CostEstimate(flops=3_000_000_000, bytes_accessed=16 << 20, transcendentals=0),
        name="panel_parts",
    )(matrix, z_part, y_part)


def hand_out_kernel(fix_ref, share_ref, fix_send, fix_recv):
    me_row, me_col = lax.axis_index("row"), lax.axis_index("col")
    lines = share_ref.shape[0]
    n_col = fix_ref.shape[0] // lines

    def copy(to):
        return pltpu.make_async_remote_copy(
            fix_ref.at[pl.ds(pl.multiple_of(to * lines, 8), lines)], share_ref,
            fix_send.at[to], fix_recv.at[0], device_id=(me_row, to), device_id_type=MESH,
        )

    @pl.when(me_col == 0)
    def _():
        for to in range(1, n_col):
            copy(to).start()
        share_ref[...] = fix_ref[0:lines, :]
        for to in range(1, n_col):
            copy(to).wait_send()

    @pl.when(me_col != 0)
    def _():
        pltpu.make_async_copy(share_ref, share_ref, fix_recv.at[0]).wait()


def handed_out(fix, n_col):
    dma = pltpu.SemaphoreType.DMA
    return pl.pallas_call(
        hand_out_kernel,
        out_shape=jax.ShapeDtypeStruct((fix.shape[0] // n_col, fix.shape[1]), jnp.float32),
        in_specs=[pl.BlockSpec(memory_space=pltpu.VMEM)],
        out_specs=pl.BlockSpec(memory_space=pltpu.VMEM),
        scratch_shapes=[dma((n_col,)), dma((1,))],
        compiler_params=pltpu.CompilerParams(has_side_effects=True, vmem_limit_bytes=16 << 20),
        cost_estimate=pl.CostEstimate(flops=1_000_000_000, bytes_accessed=4 << 20, transcendentals=0),
        name="handed_out",
    )(fix)


def per_device(front, child_tiles, tile_target, tile_count, probe):
    n_row, n_col = lax.axis_size("row"), lax.axis_size("col")
    devices = n_row * n_col
    me_row, me_col = lax.axis_index("row"), lax.axis_index("col")
    rows, cols = front.shape
    tile_rows, tile_cols = rows // TB, cols // TB
    grid = tile_cols * n_col
    held = child_tiles.shape[0]
    start = PANELS * NB
    slot_index = jnp.arange(held, dtype=jnp.int32)
    live = slot_index % SLOTS < tile_count[slot_index // SLOTS]
    first_row, first_col = tile_target // grid, tile_target % grid
    target_row = jnp.concatenate([first_row, first_col])
    target_col = jnp.concatenate([first_col, first_row])
    owner = target_row // tile_rows * n_col + target_col // tile_cols
    in_row, in_col = target_row % tile_rows, target_col % tile_cols
    upright = jnp.arange(2 * held) < held
    upright_code = 2 * (in_col // 2 * tile_rows + in_row) + in_col % 2
    blocks = cols // LANES * tile_rows
    flips = -(-rows // LANES) * tile_cols
    turned_code = 2 * (blocks + in_row // 2 * tile_cols + in_col) + in_row % 2
    code = jnp.where(upright, upright_code, turned_code)
    code = jnp.where(jnp.concatenate([live, live]), code, 2 * (blocks + flips))
    order = jnp.arange(2 * held, dtype=jnp.int32)
    same = (owner[:, None] == owner[None, :]) & (order[None, :] < order[:, None])
    slot = 2 * owner + jnp.sum(same.astype(jnp.int32), axis=1)
    at_slot = slot[None, :] == order[:, None]
    source = jnp.sum(jnp.where(at_slot, (order % held)[None, :], 0), axis=1)
    sent_code = jnp.sum(jnp.where(at_slot, code[None, :], 0), axis=1)
    outgoing = packed(child_tiles, source)
    chunks = outgoing.shape[1]
    code_lines = jnp.pad(sent_code.reshape(devices, 1, 2), ((0, 0), (0, 0), (0, LANES - 2)))
    incoming, landing, probe_rows = exchanged(
        outgoing.reshape(devices, 2 * chunks, LANES), code_lines, probe, rows
    )
    matrix = placed(front, incoming.reshape(2 * devices, chunks, LANES), landing[:, 0, :2].reshape(-1))

    global_rows = me_row * rows + jnp.arange(rows, dtype=jnp.int32)
    global_cols = me_col * cols + jnp.arange(cols, dtype=jnp.int32)
    by_cols = jnp.where((global_cols >= start)[:, None], probe, 0.0)
    by_rows = jnp.where((global_rows >= start)[:, None], probe_rows, 0.0)
    y_part = lax.dot_general(by_cols, matrix, (((0,), (1,)), ((), ())), precision=GOOD)
    panel = matrix[:, :start]
    z_part = lax.dot_general(by_rows, panel, (((0,), (0,)), ((), ())), precision=GOOD)
    inverse, solved, panel_factor, z_all, y_own = panel_parts(matrix, z_part, y_part, start, n_row, n_col)
    weights = lax.dot_general(
        z_all, inverse.reshape(start, start), (((1,), (1,)), ((), ())), precision=GOOD
    )
    fix = lax.dot_general(
        weights.reshape(-1, n_col, start // n_col), solved, (((1, 2), (0, 2)), ((), ())), precision=GOOD
    )
    fix_own = handed_out(fix, n_col)
    sketch = jnp.where((global_rows >= start)[:, None], (y_own - fix_own).T, 0.0)
    return (panel_factor, sketch)


def solution(mesh):
    return jax.shard_map(
        per_device,
        mesh=mesh,
        in_specs=(
            P("row", "col"),
            P(("row", "col"), None),
            P(("row", "col")),
            P(("row", "col")),
            P("col", None),
        ),
        out_specs=(P("row", "col"), P("row", "col")),
        check_vma=False,
    )
```

```python
import functools

import jax
import jax.numpy as jnp
from jax import lax
from jax.experimental import pallas as pl
from jax.experimental.pallas import tpu as pltpu
from jax.sharding import PartitionSpec as P

NB = 512
PANELS = 2
TB = 64
SLOTS = 32
LANES = 128
SUB = 16
BLK = 128

HIGH = lax.Precision.HIGHEST
GOOD = lax.Precision.HIGH


def pack_kernel(source_ref, tiles_ref, out_ref, laid_ref, *, pitch, unroll):
    held = tiles_ref.shape[0]
    chunks = tiles_ref.shape[1] // LANES
    for group in range(held // 8):
        for part in range(chunks):
            laid_ref[pl.ds(group * 8 * pitch + part, 8, stride=pitch), :] = tiles_ref[
                group * 8 : group * 8 + 8, part * LANES : (part + 1) * LANES
            ]

    def step(q, carry):
        start = pl.multiple_of(source_ref[q] * pitch, 8)
        out_ref[q] = laid_ref[pl.ds(start, chunks), :]
        return carry

    lax.fori_loop(0, out_ref.shape[0], step, 0, unroll=unroll)


def packed(tiles, source):
    held, width = tiles.shape
    chunks = width // LANES
    pitch = chunks + 8
    return pl.pallas_call(
        functools.partial(pack_kernel, pitch=pitch, unroll=4),
        out_shape=jax.ShapeDtypeStruct((source.shape[0], chunks, LANES), jnp.float32),
        in_specs=[pl.BlockSpec(memory_space=pltpu.SMEM), pl.BlockSpec(memory_space=pltpu.VMEM)],
        out_specs=pl.BlockSpec(memory_space=pltpu.VMEM),
        scratch_shapes=[pltpu.VMEM((held * pitch, LANES), jnp.float32)],
        compiler_params=pltpu.CompilerParams(vmem_limit_bytes=32 << 20),
        cost_estimate=pl.CostEstimate(flops=10_000_000, bytes_accessed=6 << 20, transcendentals=0),
        name="packed_tiles",
    )(source, tiles)


def place_kernel(code_ref, tiles_ref, front_ref, out_ref, sum_ref, *, unroll):
    rows, cols = front_ref.shape
    blocks = cols // LANES
    flips = -(-rows // LANES)
    half_rows = TB * TB // LANES
    sum_ref[...] = jnp.zeros_like(sum_ref)
    left = lax.broadcasted_iota(jnp.int32, (half_rows, LANES), 1) < TB

    def step(q, carry):
        code = code_ref[q]
        start = pl.multiple_of((code // 2) * TB, TB)
        odd = code % 2
        tile = tiles_ref[q]
        turned = pltpu.roll(tile, TB, 1)
        is_left = odd == 0
        keep = left == is_left
        upper = jnp.where(keep, jnp.where(is_left, tile, turned), 0.0)
        lower = jnp.where(keep, jnp.where(is_left, turned, tile), 0.0)
        even = pl.ds(start, half_rows, stride=2)
        uneven = pl.ds(start + 1, half_rows, stride=2)
        sum_ref[even, :] = sum_ref[even, :] + upper
        sum_ref[uneven, :] = sum_ref[uneven, :] + lower
        return carry

    lax.fori_loop(0, tiles_ref.shape[0], step, 0, unroll=unroll)
    for block in range(blocks):
        lo, hi = block * LANES, (block + 1) * LANES
        out_ref[:, lo:hi] = front_ref[:, lo:hi] + sum_ref[block * rows : (block + 1) * rows, :]
        for flip in range(flips):
            at = blocks * rows + flip * cols + lo
            size = min(LANES, rows - flip * LANES)
            span = slice(flip * LANES, flip * LANES + size)
            out_ref[span, lo:hi] = out_ref[span, lo:hi] + sum_ref[at : at + LANES, :].T[:size, :]


def placed(front, tiles, code):
    rows, cols = front.shape
    total = (cols // LANES) * rows + -(-rows // LANES) * cols + TB
    return pl.pallas_call(
        functools.partial(place_kernel, unroll=8),
        out_shape=jax.ShapeDtypeStruct(front.shape, jnp.float32),
        in_specs=[pl.BlockSpec(memory_space=pltpu.SMEM)] + [pl.BlockSpec(memory_space=pltpu.VMEM)] * 2,
        out_specs=pl.BlockSpec(memory_space=pltpu.VMEM),
        scratch_shapes=[pltpu.VMEM((total, LANES), jnp.float32)],
        compiler_params=pltpu.CompilerParams(vmem_limit_bytes=32 << 20),
        cost_estimate=pl.CostEstimate(flops=10_000_000, bytes_accessed=10 << 20, transcendentals=0),
        name="placed_tiles",
    )(code, tiles, front)


MESH = pl.DeviceIdType.MESH


def exchange_kernel(
    tiles_ref, code_ref, probe_ref, tiles_in, code_in, probe_rows,
    tiles_send, tiles_recv, code_send, code_recv, probe_send, probe_recv,
):
    n_row, n_col = lax.axis_size("row"), lax.axis_size("col")
    devices = n_row * n_col
    me_row, me_col = lax.axis_index("row"), lax.axis_index("col")
    me = me_row * n_col + me_col
    rows = probe_rows.shape[0]
    group = n_row // n_col
    at = pl.ds(pl.multiple_of(lax.rem(me_row, group) * rows, 8), rows)

    def copies(step):
        turn = lax.rem(step * 53, devices)
        across = lax.rem(me_row // 4 + turn // 32, n_row // 4)
        deep = lax.rem(me_row + turn // 8, 4)
        up = lax.rem(me_col // 2 + lax.rem(turn // 2, n_col // 2), n_col // 2)
        where_to = (across * 4 + deep, up * 2 + lax.rem(me_col + turn, 2))
        to = where_to[0] * n_col + where_to[1]
        return (
            pltpu.make_async_remote_copy(
                code_ref.at[to], code_in.at[me], code_send, code_recv,
                device_id=where_to, device_id_type=MESH,
            ),
            pltpu.make_async_remote_copy(
                tiles_ref.at[to], tiles_in.at[me], tiles_send, tiles_recv,
                device_id=where_to, device_id_type=MESH,
            ),
        )

    def begin(step, carry):
        for copy in copies(step):
            copy.start()
        return carry

    probe_copy = pltpu.make_async_remote_copy(
        probe_ref.at[at], probe_rows, probe_send, probe_recv, device_id=(me_row, 0), device_id_type=MESH
    )
    source_col = me_row // group
    sends_probe = (me_col == source_col) & (me_col != 0)
    gets_probe = (me_col == 0) & (source_col != 0)

    lax.fori_loop(1, devices, begin, 0)

    @pl.when(sends_probe)
    def _():
        probe_copy.start()

    @pl.when((me_col == 0) & (source_col == 0))
    def _():
        probe_rows[...] = probe_ref[at, :]

    tiles_in[me] = tiles_ref[me]
    code_in[me] = code_ref[me]
    others = pl.ds(0, devices - 1)

    def all_of(ref, sem):
        pltpu.make_async_copy(ref.at[others], ref.at[others], sem).wait()

    all_of(code_in, code_recv)
    all_of(tiles_in, tiles_recv)
    all_of(code_ref, code_send)
    all_of(tiles_ref, tiles_send)

    @pl.when(gets_probe)
    def _():
        pltpu.make_async_copy(probe_rows, probe_rows, probe_recv).wait()

    @pl.when(sends_probe)
    def _():
        probe_copy.wait_send()


def exchanged(tiles, code, probe, rows):
    dma = pltpu.SemaphoreType.DMA
    return pl.pallas_call(
        exchange_kernel,
        out_shape=(
            jax.ShapeDtypeStruct(tiles.shape, jnp.float32),
            jax.ShapeDtypeStruct(code.shape, jnp.int32),
            jax.ShapeDtypeStruct((rows, probe.shape[1]), jnp.float32),
        ),
        in_specs=[pl.BlockSpec(memory_space=pltpu.VMEM)] * 3,
        out_specs=[pl.BlockSpec(memory_space=pltpu.VMEM)] * 3,
        scratch_shapes=[dma] * 6,
        compiler_params=pltpu.CompilerParams(has_side_effects=True, vmem_limit_bytes=32 << 20),
        cost_estimate=pl.CostEstimate(flops=1_000_000_000, bytes_accessed=16 << 20, transcendentals=0),
        name="exchanged_tiles",
    )(tiles, code, probe)


def factor_rows(rows, base):
    sub = lax.broadcasted_iota(jnp.int32, (8, BLK), 0)
    lane = lax.broadcasted_iota(jnp.int32, (8, BLK), 1)

    def column(g, i):
        here = jnp.where(lane == base + i, rows[g][:, :BLK], 0.0)
        return jnp.broadcast_to(jnp.sum(here, axis=1, keepdims=True), (8, BLK))

    spread = [[column(g, i) if i < 8 * g + 8 else None for i in range(SUB)] for g in range(2)]
    halves = [[row[:, :BLK], row[:, BLK:]] for row in rows]
    for i in range(SUB):
        own, at = divmod(i, 8)
        pivot = jnp.broadcast_to(spread[own][i][at : at + 1, :], (8, BLK))
        scale = lax.rsqrt(pivot)
        lows = [None, None]
        for g in range(own, 2):
            low = spread[g][i] * scale
            lows[g] = jnp.where(sub > at, low, 0.0) if g == own else low
        for j in range(i + 1, SUB):
            g_j, at_j = divmod(j, 8)
            factor = jnp.broadcast_to(lows[g_j][at_j : at_j + 1, :], (8, BLK))
            for g in range(g_j, 2):
                spread[g][j] = spread[g][j] - lows[g] * factor
        for h in range(2):
            line = jnp.broadcast_to(halves[own][h][at : at + 1, :], (8, BLK)) * scale
            for g in range(own, 2):
                new = halves[g][h] - lows[g] * line
                halves[g][h] = jnp.where(sub == at, line, new) if g == own else new
    return [jnp.concatenate(half, axis=1) for half in halves]


def inverse_factor(x_ref, beside):
    row = lax.broadcasted_iota(jnp.int32, (BLK, 2 * BLK), 0)

    def step(s, carry):
        base = pl.multiple_of(s * SUB, SUB)
        rows = factor_rows([x_ref[pl.ds(base, 8), :], x_ref[pl.ds(base + 8, 8), :]], base)
        beside(s)
        x_ref[pl.ds(base, 8), :] = rows[0]
        x_ref[pl.ds(base + 8, 8), :] = rows[1]
        done = jnp.concatenate(rows, axis=0)
        gone = plain_dot(done[:, :BLK].T, done)
        x_ref[...] = x_ref[...] - jnp.where(row >= base + SUB, gone, 0.0)
        return carry

    lax.fori_loop(0, BLK // SUB, step, 0)


def plain_dot(a, b):
    return lax.dot_general(
        a, b, (((1,), (0,)), ((), ())), precision=HIGH, preferred_element_type=jnp.float32
    )


def halves_of(a):
    top = a.astype(jnp.bfloat16)
    return top, (a - top.astype(jnp.float32)).astype(jnp.bfloat16)


def turned_dot(a, b):
    a_top, a_rest = halves_of(a)
    b_top, b_rest = halves_of(b)

    def part(p, q):
        return lax.dot_general(p, q, (((1,), (1,)), ((), ())), preferred_element_type=jnp.float32)

    return part(a_top, b_top) + (part(a_top, b_rest) + part(a_rest, b_top))


def panel_kernel(
    matrix_ref, z_ref, y_ref, panel_ref, y_own_ref, share_ref,
    w_ref, solved_ref, z_all_ref, fix_ref, m_ref, stage_ref, x_ref, z_in, y_in,
    first_send, first_recv, next_send, d_recv, z_send, z_recv, zall_send, zall_recv,
    y_send, y_recv, s_send, s_recv, fix_send, fix_recv,
):
    me_row, me_col = lax.axis_index("row"), lax.axis_index("col")
    n_row, n_col = z_in.shape[0], y_in.shape[0]
    blocks, _, order = m_ref.shape
    rows = matrix_ref.shape[0]
    piece = BLK // n_row
    z_lines, y_lines = z_in.shape[1], y_in.shape[1]
    on_panel = me_col == 0

    def partner(step):
        turn = lax.rem(step * 7, n_row)
        side = 4
        across = lax.rem(me_row // side + turn // side, n_row // side)
        return across * side + lax.rem(lax.rem(me_row, side) + lax.rem(turn, side), side)

    def y_copy(step):
        to = lax.rem(me_col + step, n_col)
        return pltpu.make_async_remote_copy(
            y_ref.at[pl.ds(pl.multiple_of(to * y_lines, 8), y_lines)], y_in.at[me_col],
            y_send.at[to], y_recv.at[me_col], device_id=(me_row, to), device_id_type=MESH,
        )

    def z_copy(step):
        to = partner(step)
        return pltpu.make_async_remote_copy(
            z_ref.at[pl.ds(pl.multiple_of(to * z_lines, 8), z_lines)], z_in.at[me_row],
            z_send.at[to], z_recv.at[me_row], device_id=(to, me_col), device_id_type=MESH,
        )

    def z_all_copy(step):
        to = partner(step)
        mine = z_all_ref.at[pl.ds(pl.multiple_of(me_row * z_lines, 8), z_lines)]
        return pltpu.make_async_remote_copy(
            mine, mine, zall_send.at[to], zall_recv.at[me_row], device_id=(to, me_col), device_id_type=MESH,
        )

    def solved_copy(i):
        return pltpu.make_async_remote_copy(
            solved_ref.at[i], panel_ref, s_send.at[i], s_recv.at[0],
            device_id=(me_row, i), device_id_type=MESH,
        )

    def fix_copy(to):
        return pltpu.make_async_remote_copy(
            fix_ref.at[to * y_lines : (to + 1) * y_lines], share_ref, fix_send.at[to], fix_recv.at[0],
            device_id=(me_row, to), device_id_type=MESH,
        )

    def arrived(into, sem):
        pltpu.make_async_copy(into, into, sem).wait()

    def first_copy(b, to, root):
        at = b * BLK + to * piece - root * rows
        return pltpu.make_async_remote_copy(
            matrix_ref.at[pl.ds(pl.multiple_of(at, 8), piece), b * BLK : order],
            stage_ref.at[b, :, b * BLK : order],
            first_send.at[b], first_recv.at[b], device_id=(to, me_col), device_id_type=MESH,
        )

    own_lines = pl.ds(pl.multiple_of(me_row * piece, 8), piece)

    def held_piece(b, root=None):
        if root is None:
            return stage_ref.at[b, :, b * BLK : order]
        at = b * BLK + root * piece - root * rows
        return matrix_ref.at[at : at + piece, b * BLK : order]

    def next_copy(b, step, root=None):
        to = partner(step)
        return pltpu.make_async_remote_copy(
            held_piece(b, root), m_ref.at[b, own_lines, b * BLK : order], next_send.at[b], d_recv.at[b],
            device_id=(to, me_col), device_id_type=MESH,
        )

    def pieces_of(b, count):
        return m_ref.at[b, 0 : count * piece, b * BLK : order]

    def each(count, action):
        def step(s, carry):
            action(s)
            return carry

        lax.fori_loop(1, count, step, 0)

    n_roots = -(-order // rows)
    sent = [[] for _ in range(n_roots)]
    for root in range(n_roots):
        for b in range(blocks):
            first = max(0, root * rows - b * BLK) // piece
            last = min(BLK, (root + 1) * rows - b * BLK) // piece
            if first < last:
                sent[root].append((b, first, last))

    for root in range(n_roots):
        @pl.when(on_panel & (me_row == root))
        def _(root=root):
            for b, first, last in sent[root]:
                for to in range(first, last):
                    if to != root:
                        first_copy(b, to, root).start()

    local = [[b for b, first, last in sent[root] if first <= root < last] for root in range(n_roots)]
    for b in range(blocks):
        mine = None
        for root in range(n_roots):
            if b in local[root]:
                mine = root

        @pl.when(on_panel & (me_row != mine))
        def _(b=b):
            arrived(held_piece(b), first_recv.at[b])
            each(n_row, lambda s: next_copy(b, s).start())
            m_ref[b, own_lines, b * BLK : order] = stage_ref[b, :, b * BLK : order]

        @pl.when(on_panel & (me_row == mine))
        def _(b=b, mine=mine):
            each(n_row, lambda s: next_copy(b, s, mine).start())
            at = b * BLK + mine * piece - mine * rows
            m_ref[b, own_lines, b * BLK : order] = matrix_ref[at : at + piece, b * BLK : order]

    each(n_col, lambda s: y_copy(s).start())

    def sum_z():
        own = pl.ds(pl.multiple_of(me_row * z_lines, 8), z_lines)
        z_in[me_row] = z_ref[own, :]

        def wait_z(s):
            k = lax.rem(me_row + s, n_row)
            arrived(z_in.at[k], z_recv.at[k])

        each(n_row, wait_z)
        total = z_in[0]
        for k in range(1, n_row):
            total = total + z_in[k]
        z_all_ref[own, :] = total

    def sum_y():
        def wait_y(s):
            k = lax.rem(me_col + s, n_col)
            arrived(y_in.at[k], y_recv.at[k])

        each(n_col, wait_y)
        y_in[me_col] = y_ref[pl.ds(pl.multiple_of(me_col * y_lines, 8), y_lines), :]
        y_total = y_in[0]
        for k in range(1, n_col):
            y_total = y_total + y_in[k]
        y_own_ref[...] = y_total

    eye = (
        lax.broadcasted_iota(jnp.int32, (BLK, BLK), 0) == lax.broadcasted_iota(jnp.int32, (BLK, BLK), 1)
    ).astype(jnp.float32)
    slab = rows // (BLK // SUB)

    def solve_slab(i, s):
        lines = pl.ds(pl.multiple_of(s * slab, 8), slab)
        hi = (i + 1) * BLK
        part = turned_dot(matrix_ref[lines, :hi], w_ref[i, :, :hi])
        if i * BLK >= NB:
            line = me_row * rows + s * slab + lax.broadcasted_iota(jnp.int32, (slab, BLK), 0)
            part = jnp.where(line >= i * BLK // NB * NB, part, 0.0)
        solved_ref[i, lines, :] = part

    @pl.when(on_panel)
    def _():
        for i in range(blocks):
            lo, hi = i * BLK, (i + 1) * BLK
            arrived(pieces_of(i, n_row - 1), d_recv.at[i])
            if i == 1:
                each(n_row, lambda s: z_copy(s).start())
            own_row = m_ref[i, :, lo:]
            if i:
                left = jnp.concatenate([m_ref[b, :, lo:hi].T for b in range(i)], axis=1)
                own_row = own_row - plain_dot(left, m_ref[:i, :, lo:].reshape(lo, order - lo))
                w_ref[i, :, :lo] = -plain_dot(left, w_ref[:i, :, :lo].reshape(lo, lo))
            diag = own_row[:, :BLK]
            x_ref[:, :BLK] = 0.5 * (diag + diag.T)
            x_ref[:, BLK:] = eye
            if hi < order:
                m_ref[i, :, hi:] = own_row[:, BLK:]
            inverse_factor(x_ref, (lambda s: solve_slab(i - 1, s)) if i else (lambda s: None))
            if i > 1:
                solved_copy(i - 1).start()
            if i == 4:
                sum_z()
            w_diag = x_ref[:, BLK:]
            w_ref[i, :, lo:hi] = w_diag
            if i:
                w_ref[i, :, :lo] = plain_dot(w_diag, w_ref[i, :, :lo])
            if hi < order:
                m_ref[i, :, hi:] = plain_dot(w_diag, m_ref[i, :, hi:])
                w_ref[i, :, hi:] = jnp.zeros((BLK, order - hi), jnp.float32)
            if i == 4:
                each(n_row, lambda s: z_all_copy(s).start())

        def last(s, carry):
            solve_slab(blocks - 1, s)
            return carry

        lax.fori_loop(0, BLK // SUB, last, 0)

    sum_y()

    @pl.when(on_panel)
    def _():
        solved_copy(blocks - 1).start()
        panel_ref[...] = solved_ref[0]

        def wait_all(s):
            k = lax.rem(me_row + s, n_row)
            lines = z_all_ref.at[pl.ds(pl.multiple_of(k * z_lines, 8), z_lines)]
            arrived(lines, zall_recv.at[k])

        each(n_row, wait_all)
        inverse = w_ref[...].reshape(order, order)
        weights = turned_dot(z_all_ref[...], inverse)
        half = fix_ref.shape[0] // 2
        for part in (1, 0):
            lines = slice(part * half, (part + 1) * half)
            total = None
            for i in range(blocks):
                term = turned_dot(weights[lines, i * BLK : (i + 1) * BLK], solved_ref[i])
                total = term if total is None else total + term
            fix_ref[lines, :] = total
            for to in range(part * n_col // 2, (part + 1) * n_col // 2):
                if to:
                    fix_copy(to).start()
        share_ref[...] = fix_ref[0:y_lines, :]
        each(n_row, lambda s: z_copy(s).wait_send())
        each(n_row, lambda s: z_all_copy(s).wait_send())
        each(n_col, lambda s: solved_copy(s).wait_send())
        for to in range(1, n_col):
            fix_copy(to).wait_send()
        for b in range(blocks):
            arrived(pieces_of(b, n_row - 1), next_send.at[b])

    @pl.when(me_col != 0)
    def _():
        arrived(panel_ref, s_recv.at[0])
        arrived(share_ref, fix_recv.at[0])

    each(n_col, lambda s: y_copy(s).wait_send())
    for root in range(n_roots):
        @pl.when(on_panel & (me_row == root))
        def _(root=root):
            for b, first, last in sent[root]:
                count = last - first - (first <= root < last)
                arrived(pieces_of(b, count), first_send.at[b])


def panel_parts(matrix, z_part, y_part, order, n_row, n_col):
    lines_z, lines_y = z_part.shape[0] // n_row, y_part.shape[0] // n_col
    rows = matrix.shape[0]
    width = order // n_col
    dma = pltpu.SemaphoreType.DMA
    whole = functools.partial(jax.ShapeDtypeStruct, dtype=jnp.float32)
    return pl.pallas_call(
        panel_kernel,
        out_shape=(
            whole((rows, width)),
            whole((lines_y, y_part.shape[1])),
            whole((lines_y, y_part.shape[1])),
        ),
        in_specs=[pl.BlockSpec(memory_space=pltpu.VMEM)] * 3,
        out_specs=[pl.BlockSpec(memory_space=pltpu.VMEM)] * 3,
        scratch_shapes=[
            pltpu.VMEM((order // BLK, BLK, order), jnp.float32),
            pltpu.VMEM((n_col, rows, width), jnp.float32),
            pltpu.VMEM(z_part.shape, jnp.float32),
            pltpu.VMEM(y_part.shape, jnp.float32),
            pltpu.VMEM((order // BLK, BLK, order), jnp.float32),
            pltpu.VMEM((order // BLK, BLK // n_row, order), jnp.float32),
            pltpu.VMEM((BLK, 2 * BLK), jnp.float32),
            pltpu.VMEM((n_row, lines_z, z_part.shape[1]), jnp.float32),
            pltpu.VMEM((n_col, lines_y, y_part.shape[1]), jnp.float32),
            *[dma((order // BLK,))] * 4,
            *[dma((n_row,))] * 4,
            *[dma((n_col,))] * 3, dma((1,)), dma((n_col,)), dma((1,)),
        ],
        compiler_params=pltpu.CompilerParams(has_side_effects=True, vmem_limit_bytes=60 << 20),
        cost_estimate=pl.CostEstimate(flops=3_000_000_000, bytes_accessed=16 << 20, transcendentals=0),
        name="panel_parts",
    )(matrix, z_part, y_part)


def per_device(front, child_tiles, tile_target, tile_count, probe):
    n_row, n_col = lax.axis_size("row"), lax.axis_size("col")
    devices = n_row * n_col
    me_row, me_col = lax.axis_index("row"), lax.axis_index("col")
    rows, cols = front.shape
    tile_rows, tile_cols = rows // TB, cols // TB
    grid = tile_cols * n_col
    held = child_tiles.shape[0]
    start = PANELS * NB
    slot_index = jnp.arange(held, dtype=jnp.int32)
    live = slot_index % SLOTS < tile_count[slot_index // SLOTS]
    first_row, first_col = tile_target // grid, tile_target % grid
    target_row = jnp.concatenate([first_row, first_col])
    target_col = jnp.concatenate([first_col, first_row])
    owner = target_row // tile_rows * n_col + target_col // tile_cols
    in_row, in_col = target_row % tile_rows, target_col % tile_cols
    upright = jnp.arange(2 * held) < held
    upright_code = 2 * (in_col // 2 * tile_rows + in_row) + in_col % 2
    blocks = cols // LANES * tile_rows
    flips = -(-rows // LANES) * tile_cols
    turned_code = 2 * (blocks + in_row // 2 * tile_cols + in_col) + in_row % 2
    code = jnp.where(upright, upright_code, turned_code)
    code = jnp.where(jnp.concatenate([live, live]), code, 2 * (blocks + flips))
    order = jnp.arange(2 * held, dtype=jnp.int32)
    same = (owner[:, None] == owner[None, :]) & (order[None, :] < order[:, None])
    slot = 2 * owner + jnp.sum(same.astype(jnp.int32), axis=1)
    at_slot = slot[None, :] == order[:, None]
    source = jnp.sum(jnp.where(at_slot, (order % held)[None, :], 0), axis=1)
    sent_code = jnp.sum(jnp.where(at_slot, code[None, :], 0), axis=1)
    outgoing = packed(child_tiles, source)
    chunks = outgoing.shape[1]
    code_lines = jnp.pad(sent_code.reshape(devices, 1, 2), ((0, 0), (0, 0), (0, LANES - 2)))
    incoming, landing, probe_rows = exchanged(
        outgoing.reshape(devices, 2 * chunks, LANES), code_lines, probe, rows
    )
    matrix = placed(front, incoming.reshape(2 * devices, chunks, LANES), landing[:, 0, :2].reshape(-1))

    global_rows = me_row * rows + jnp.arange(rows, dtype=jnp.int32)
    global_cols = me_col * cols + jnp.arange(cols, dtype=jnp.int32)
    by_cols = jnp.where((global_cols >= start)[:, None], probe, 0.0)
    by_rows = jnp.where((global_rows >= start)[:, None], probe_rows, 0.0)
    y_part = lax.dot_general(by_cols, matrix, (((0,), (1,)), ((), ())), precision=GOOD)
    panel = matrix[:, :start]
    z_part = lax.dot_general(by_rows, panel, (((0,), (0,)), ((), ())), precision=GOOD)
    panel_factor, y_own, fix_own = panel_parts(matrix, z_part, y_part, start, n_row, n_col)
    sketch = jnp.where((global_rows >= start)[:, None], (y_own - fix_own).T, 0.0)
    return (panel_factor, sketch)


def solution(mesh):
    return jax.shard_map(
        per_device,
        mesh=mesh,
        in_specs=(
            P("row", "col"),
            P(("row", "col"), None),
            P(("row", "col")),
            P(("row", "col")),
            P("col", None),
        ),
        out_specs=(P("row", "col"), P("row", "col")),
        check_vma=False,
    )
```

```python
import functools

import jax
import jax.numpy as jnp
from jax import lax
from jax.experimental import pallas as pl
from jax.experimental.pallas import tpu as pltpu
from jax.sharding import PartitionSpec as P

NB = 512
PANELS = 2
TB = 64
SLOTS = 32
LANES = 128
SUB = 32
GROUP = 32
BLK = 128


def pack_kernel(source_ref, tiles_ref, out_ref, laid_ref, *, pitch, unroll):
    held = tiles_ref.shape[0]
    chunks = tiles_ref.shape[1] // LANES
    for group in range(held // 8):
        for part in range(chunks):
            laid_ref[pl.ds(group * 8 * pitch + part, 8, stride=pitch), :] = tiles_ref[
                group * 8 : group * 8 + 8, part * LANES : (part + 1) * LANES
            ]

    def step(q, carry):
        start = pl.multiple_of(source_ref[q] * pitch, 8)
        out_ref[q] = laid_ref[pl.ds(start, chunks), :]
        return carry

    lax.fori_loop(0, out_ref.shape[0], step, 0, unroll=unroll)


def packed(tiles, source):
    held, width = tiles.shape
    chunks = width // LANES
    pitch = chunks + 8
    return pl.pallas_call(
        functools.partial(pack_kernel, pitch=pitch, unroll=4),
        out_shape=jax.ShapeDtypeStruct((source.shape[0], chunks, LANES), jnp.float32),
        in_specs=[pl.BlockSpec(memory_space=pltpu.SMEM), pl.BlockSpec(memory_space=pltpu.VMEM)],
        out_specs=pl.BlockSpec(memory_space=pltpu.VMEM),
        scratch_shapes=[pltpu.VMEM((held * pitch, LANES), jnp.float32)],
        compiler_params=pltpu.CompilerParams(vmem_limit_bytes=60 << 20),
        cost_estimate=pl.CostEstimate(flops=10_000_000, bytes_accessed=6 << 20, transcendentals=0),
        name="packed_tiles",
    )(source, tiles)


def place_kernel(code_ref, tiles_ref, front_hbm, out_ref, sum_ref, front_ref, front_sem, *, unroll):
    rows, cols = front_ref.shape
    blocks = cols // LANES
    flips = -(-rows // LANES)
    half_rows = TB * TB // LANES
    group, groups = pl.program_id(0), pl.num_programs(0)
    count = tiles_ref.shape[0]
    front_copy = pltpu.make_async_copy(front_hbm, front_ref, front_sem)

    @pl.when(group == 0)
    def _():
        front_copy.start()
        sum_ref[...] = jnp.zeros_like(sum_ref)

    left = lax.broadcasted_iota(jnp.int32, (half_rows, LANES), 1) < TB

    def step(q, carry):
        code = code_ref[group * count + q]
        start = pl.multiple_of((code // 2) * TB, TB)
        odd = code % 2
        tile = tiles_ref[q]
        turned = pltpu.roll(tile, TB, 1)
        is_left = odd == 0
        keep = left == is_left
        upper = jnp.where(keep, jnp.where(is_left, tile, turned), 0.0)
        lower = jnp.where(keep, jnp.where(is_left, turned, tile), 0.0)
        even = pl.ds(start, half_rows, stride=2)
        uneven = pl.ds(start + 1, half_rows, stride=2)
        sum_ref[even, :] = sum_ref[even, :] + upper
        sum_ref[uneven, :] = sum_ref[uneven, :] + lower
        return carry

    lax.fori_loop(0, count, step, 0, unroll=unroll)
    @pl.when(group == groups - 1)
    def _():
        front_copy.wait()
        for block in range(blocks):
            lo, hi = block * LANES, (block + 1) * LANES
            out_ref[:, lo:hi] = front_ref[:, lo:hi] + sum_ref[block * rows : (block + 1) * rows, :]
            for flip in range(flips):
                at = blocks * rows + flip * cols + lo
                size = min(LANES, rows - flip * LANES)
                span = slice(flip * LANES, flip * LANES + size)
                out_ref[span, lo:hi] = out_ref[span, lo:hi] + sum_ref[at : at + LANES, :].T[:size, :]


def placed(front, tiles, code):
    rows, cols = front.shape
    total = (cols // LANES) * rows + -(-rows // LANES) * cols + TB
    return pl.pallas_call(
        functools.partial(place_kernel, unroll=8),
        out_shape=jax.ShapeDtypeStruct(front.shape, jnp.float32),
        grid=(tiles.shape[0] // GROUP,),
        in_specs=[
            pl.BlockSpec(memory_space=pltpu.SMEM),
            pl.BlockSpec((GROUP, *tiles.shape[1:]), lambda g: (g, 0, 0)),
            pl.BlockSpec(memory_space=pltpu.HBM),
        ],
        out_specs=pl.BlockSpec(front.shape, lambda g: (0, 0)),
        scratch_shapes=[
            pltpu.VMEM((total, LANES), jnp.float32),
            pltpu.VMEM(front.shape, jnp.float32),
            pltpu.SemaphoreType.DMA,
        ],
        compiler_params=pltpu.CompilerParams(vmem_limit_bytes=60 << 20),
        cost_estimate=pl.CostEstimate(flops=10_000_000, bytes_accessed=10 << 20, transcendentals=0),
        name="placed_tiles",
    )(code, tiles, front)


MESH = pl.DeviceIdType.MESH


def exchange_kernel(
    tiles_ref, code_ref, probe_ref, tiles_in, code_in, probe_rows,
    tiles_send, tiles_recv, code_send, code_recv, probe_send, probe_recv, own_sem,
):
    n_row, n_col = lax.axis_size("row"), lax.axis_size("col")
    devices = n_row * n_col
    me_row, me_col = lax.axis_index("row"), lax.axis_index("col")
    me = me_row * n_col + me_col
    rows = probe_rows.shape[0]
    group = n_row // n_col
    at = pl.ds(pl.multiple_of(lax.rem(me_row, group) * rows, 8), rows)

    def copies(step):
        turn = lax.rem(step * 53, devices)
        across = lax.rem(me_row // 4 + turn // 32, n_row // 4)
        deep = lax.rem(me_row + turn // 8, 4)
        up = lax.rem(me_col // 2 + lax.rem(turn // 2, n_col // 2), n_col // 2)
        where_to = (across * 4 + deep, up * 2 + lax.rem(me_col + turn, 2))
        to = where_to[0] * n_col + where_to[1]
        return (
            pltpu.make_async_remote_copy(
                code_ref.at[to], code_in.at[me], code_send, code_recv,
                device_id=where_to, device_id_type=MESH,
            ),
            pltpu.make_async_remote_copy(
                tiles_ref.at[to], tiles_in.at[me], tiles_send, tiles_recv,
                device_id=where_to, device_id_type=MESH,
            ),
        )

    def begin(step, carry):
        for copy in copies(step):
            copy.start()
        return carry

    probe_copy = pltpu.make_async_remote_copy(
        probe_ref.at[at], probe_rows, probe_send, probe_recv, device_id=(me_row, 0), device_id_type=MESH
    )
    source_col = me_row // group
    sends_probe = (me_col == source_col) & (me_col != 0)
    gets_probe = (me_col == 0) & (source_col != 0)

    lax.fori_loop(1, devices, begin, 0)

    @pl.when(sends_probe)
    def _():
        probe_copy.start()

    @pl.when((me_col == 0) & (source_col == 0))
    def _():
        probe_rows[...] = probe_ref[at, :]

    own = pltpu.make_async_copy(tiles_ref.at[me], tiles_in.at[me], own_sem)
    own.start()
    code_in[me] = code_ref[me]
    others = pl.ds(0, devices - 1)

    def all_of(ref, sem):
        pltpu.make_async_copy(ref.at[others], ref.at[others], sem).wait()

    own.wait()
    all_of(code_in, code_recv)
    all_of(tiles_in, tiles_recv)
    all_of(code_ref, code_send)
    all_of(tiles_ref, tiles_send)

    @pl.when(gets_probe)
    def _():
        pltpu.make_async_copy(probe_rows, probe_rows, probe_recv).wait()

    @pl.when(sends_probe)
    def _():
        probe_copy.wait_send()


def exchanged(tiles, code, probe, rows):
    dma = pltpu.SemaphoreType.DMA
    return pl.pallas_call(
        exchange_kernel,
        out_shape=(
            jax.ShapeDtypeStruct(tiles.shape, jnp.float32),
            jax.ShapeDtypeStruct(code.shape, jnp.int32),
            jax.ShapeDtypeStruct((rows, probe.shape[1]), jnp.float32),
        ),
        in_specs=[pl.BlockSpec(memory_space=pltpu.HBM)] + [pl.BlockSpec(memory_space=pltpu.VMEM)] * 2,
        out_specs=[pl.BlockSpec(memory_space=pltpu.HBM)] + [pl.BlockSpec(memory_space=pltpu.VMEM)] * 2,
        scratch_shapes=[dma] * 7,
        compiler_params=pltpu.CompilerParams(has_side_effects=True, vmem_limit_bytes=60 << 20),
        cost_estimate=pl.CostEstimate(flops=1_000_000_000, bytes_accessed=16 << 20, transcendentals=0),
        name="exchanged_tiles",
    )(tiles, code, probe)


def factor_rows(rows, base):
    groups = len(rows)
    sub = lax.broadcasted_iota(jnp.int32, (8, BLK), 0)
    lane = lax.broadcasted_iota(jnp.int32, (8, BLK), 1)

    def column(g, i):
        here = jnp.where(lane == base + i, rows[g][:, :BLK], 0.0)
        return jnp.broadcast_to(jnp.sum(here, axis=1, keepdims=True), (8, BLK))

    spread = [[column(g, i) if i < 8 * g + 8 else None for i in range(SUB)] for g in range(groups)]
    halves = [[row[:, :BLK], row[:, BLK:]] for row in rows]
    for i in range(SUB):
        own, at = divmod(i, 8)
        pivot = jnp.broadcast_to(spread[own][i][at : at + 1, :], (8, BLK))
        scale = lax.rsqrt(pivot)
        lows = [None] * groups
        for g in range(own, groups):
            low = spread[g][i] * scale
            lows[g] = jnp.where(sub > at, low, 0.0) if g == own else low
        for j in range(i + 1, SUB):
            g_j, at_j = divmod(j, 8)
            factor = jnp.broadcast_to(lows[g_j][at_j : at_j + 1, :], (8, BLK))
            for g in range(g_j, groups):
                spread[g][j] = spread[g][j] - lows[g] * factor
        for h in range(2):
            line = jnp.broadcast_to(halves[own][h][at : at + 1, :], (8, BLK)) * scale
            for g in range(own, groups):
                new = halves[g][h] - lows[g] * line
                halves[g][h] = jnp.where(sub == at, line, new) if g == own else new
    return [jnp.concatenate(half, axis=1) for half in halves]


def inverse_factor(x_ref, beside):
    row = lax.broadcasted_iota(jnp.int32, (BLK, 2 * BLK), 0)

    def step(s, carry):
        base = pl.multiple_of(s * SUB, SUB)
        lines = [pl.ds(base + g, 8) for g in range(0, SUB, 8)]
        rows = factor_rows([x_ref[line, :] for line in lines], base)
        beside(s)
        for line, value in zip(lines, rows):
            x_ref[line, :] = value
        done = jnp.concatenate(rows, axis=0)
        gone = joined_dot(done[:, :BLK].T, done)
        x_ref[...] = x_ref[...] - jnp.where(row >= base + SUB, gone, 0.0)
        return carry

    lax.fori_loop(0, BLK // SUB, step, 0)


def halves_of(a):
    top = a.astype(jnp.bfloat16)
    return top, (a - top.astype(jnp.float32)).astype(jnp.bfloat16)


def split_dot(a, b, b_dim):
    a_top, a_rest = halves_of(a)
    b_top, b_rest = halves_of(b)

    def part(p, q):
        return lax.dot_general(
            p, q, (((1,), (b_dim,)), ((), ())), preferred_element_type=jnp.float32
        )

    return part(a_top, b_top) + (part(a_top, b_rest) + part(a_rest, b_top))


def plain_dot(a, b):
    return split_dot(a, b, 0)


def turned_dot(a, b):
    return split_dot(a, b, 1)


def joined_dot(a, b):
    a_top, a_rest = halves_of(a)
    b_top, b_rest = halves_of(b)
    return lax.dot_general(
        jnp.concatenate([a_top, a_top, a_rest], axis=1),
        jnp.concatenate([b_top, b_rest, b_top], axis=0),
        (((1,), (0,)), ((), ())),
        preferred_element_type=jnp.float32,
    )


def panel_kernel(
    matrix_ref, probe_ref, probe_rows_ref, panel_ref, y_own_ref, share_ref,
    z_ref, y_ref, w_ref, solved_ref, z_all_ref, fix_ref, m_ref, stage_ref, x_ref, z_in, y_in,
    first_send, first_recv, next_send, d_recv, z_send, z_recv, zall_send, zall_recv,
    y_send, y_recv, s_send, s_recv, fix_send, fix_recv,
):
    me_row, me_col = lax.axis_index("row"), lax.axis_index("col")
    n_row, n_col = z_in.shape[0], y_in.shape[0]
    blocks, _, order = m_ref.shape
    rows = matrix_ref.shape[0]
    piece = BLK // n_row
    z_lines, y_lines = z_in.shape[1], y_in.shape[1]
    on_panel = me_col == 0

    def partner(step):
        turn = lax.rem(step * 7, n_row)
        side = 4
        across = lax.rem(me_row // side + turn // side, n_row // side)
        return across * side + lax.rem(lax.rem(me_row, side) + lax.rem(turn, side), side)

    def y_copy(step):
        to = lax.rem(me_col + step, n_col)
        return pltpu.make_async_remote_copy(
            y_ref.at[pl.ds(pl.multiple_of(to * y_lines, 8), y_lines)], y_in.at[me_col],
            y_send.at[to], y_recv.at[me_col], device_id=(me_row, to), device_id_type=MESH,
        )

    def z_copy(step):
        to = partner(step)
        return pltpu.make_async_remote_copy(
            z_ref.at[pl.ds(pl.multiple_of(to * z_lines, 8), z_lines)], z_in.at[me_row],
            z_send.at[to], z_recv.at[me_row], device_id=(to, me_col), device_id_type=MESH,
        )

    def z_all_copy(step):
        to = partner(step)
        mine = z_all_ref.at[pl.ds(pl.multiple_of(me_row * z_lines, 8), z_lines)]
        return pltpu.make_async_remote_copy(
            mine, mine, zall_send.at[to], zall_recv.at[me_row], device_id=(to, me_col), device_id_type=MESH,
        )

    def solved_copy(i):
        return pltpu.make_async_remote_copy(
            solved_ref.at[i], panel_ref, s_send.at[i], s_recv.at[0],
            device_id=(me_row, i), device_id_type=MESH,
        )

    def fix_copy(to):
        return pltpu.make_async_remote_copy(
            fix_ref.at[to * y_lines : (to + 1) * y_lines], share_ref, fix_send.at[to], fix_recv.at[0],
            device_id=(me_row, to), device_id_type=MESH,
        )

    def arrived(into, sem):
        pltpu.make_async_copy(into, into, sem).wait()

    def first_copy(b, to, root):
        at = b * BLK + to * piece - root * rows
        return pltpu.make_async_remote_copy(
            matrix_ref.at[pl.ds(pl.multiple_of(at, 8), piece), b * BLK : order],
            stage_ref.at[b, :, b * BLK : order],
            first_send.at[b], first_recv.at[b], device_id=(to, me_col), device_id_type=MESH,
        )

    own_lines = pl.ds(pl.multiple_of(me_row * piece, 8), piece)

    def held_piece(b, root=None):
        if root is None:
            return stage_ref.at[b, :, b * BLK : order]
        at = b * BLK + root * piece - root * rows
        return matrix_ref.at[at : at + piece, b * BLK : order]

    def next_copy(b, step, root=None):
        to = partner(step)
        return pltpu.make_async_remote_copy(
            held_piece(b, root), m_ref.at[b, own_lines, b * BLK : order], next_send.at[b], d_recv.at[b],
            device_id=(to, me_col), device_id_type=MESH,
        )

    def pieces_of(b, count):
        return m_ref.at[b, 0 : count * piece, b * BLK : order]

    def each(count, action):
        def step(s, carry):
            action(s)
            return carry

        lax.fori_loop(1, count, step, 0)

    n_roots = -(-order // rows)
    sent = [[] for _ in range(n_roots)]
    for root in range(n_roots):
        for b in range(blocks):
            first = max(0, root * rows - b * BLK) // piece
            last = min(BLK, (root + 1) * rows - b * BLK) // piece
            if first < last:
                sent[root].append((b, first, last))

    for root in range(n_roots):
        @pl.when(on_panel & (me_row == root))
        def _(root=root):
            for b, first, last in sent[root]:
                for to in range(first, last):
                    if to != root:
                        first_copy(b, to, root).start()

    local = [[b for b, first, last in sent[root] if first <= root < last] for root in range(n_roots)]
    for b in range(blocks):
        mine = None
        for root in range(n_roots):
            if b in local[root]:
                mine = root

        @pl.when(on_panel & (me_row != mine))
        def _(b=b):
            arrived(held_piece(b), first_recv.at[b])
            each(n_row, lambda s: next_copy(b, s).start())
            m_ref[b, own_lines, b * BLK : order] = stage_ref[b, :, b * BLK : order]

        @pl.when(on_panel & (me_row == mine))
        def _(b=b, mine=mine):
            each(n_row, lambda s: next_copy(b, s, mine).start())
            at = b * BLK + mine * piece - mine * rows
            m_ref[b, own_lines, b * BLK : order] = matrix_ref[at : at + piece, b * BLK : order]

    def z_slab(s):
        lanes = pl.ds(pl.multiple_of(s * z_slab_width, BLK), z_slab_width)
        line = me_row * rows + lax.broadcasted_iota(jnp.int32, (rows, z_slab_width), 0)
        chosen = jnp.where(line >= order, probe_rows_ref[:, lanes], 0.0)
        z_ref[lanes, :] = plain_dot(chosen.T, matrix_ref[:, :order])

    def y_slab(s, first):
        lanes = pl.ds(pl.multiple_of(s * z_slab_width, BLK), z_slab_width)
        y_ref[lanes, :] = turned_dot(probe_ref[first:, lanes].T, matrix_ref[:, first:])

    steps = BLK // SUB
    z_slab_width = z_ref.shape[0] // steps

    @pl.when(me_col != 0)
    def _():
        def step(s, carry):
            y_slab(s, 0)
            return carry

        lax.fori_loop(0, steps, step, 0)
        each(n_col, lambda s: y_copy(s).start())

    def sum_z():
        own = pl.ds(pl.multiple_of(me_row * z_lines, 8), z_lines)
        z_in[me_row] = z_ref[own, :]

        def wait_z(s):
            k = lax.rem(me_row + s, n_row)
            arrived(z_in.at[k], z_recv.at[k])

        each(n_row, wait_z)
        total = z_in[0]
        for k in range(1, n_row):
            total = total + z_in[k]
        z_all_ref[own, :] = total

    def sum_y():
        def wait_y(s):
            k = lax.rem(me_col + s, n_col)
            arrived(y_in.at[k], y_recv.at[k])

        each(n_col, wait_y)
        y_in[me_col] = y_ref[pl.ds(pl.multiple_of(me_col * y_lines, 8), y_lines), :]
        y_total = y_in[0]
        for k in range(1, n_col):
            y_total = y_total + y_in[k]
        y_own_ref[...] = y_total

    eye = (
        lax.broadcasted_iota(jnp.int32, (BLK, BLK), 0) == lax.broadcasted_iota(jnp.int32, (BLK, BLK), 1)
    ).astype(jnp.float32)
    slab = rows // (BLK // SUB)

    def solve_slab(i, s):
        lines = pl.ds(pl.multiple_of(s * slab, 8), slab)
        hi = (i + 1) * BLK
        part = turned_dot(matrix_ref[lines, :hi], w_ref[i, :, :hi])
        if i * BLK >= NB:
            line = me_row * rows + s * slab + lax.broadcasted_iota(jnp.int32, (slab, BLK), 0)
            part = jnp.where(line >= i * BLK // NB * NB, part, 0.0)
        solved_ref[i, lines, :] = part

    def beside(i, s):
        if i == 0:
            z_slab(s)
        else:
            solve_slab(i - 1, s)
        if i == 1:
            y_slab(s, order)

    @pl.when(on_panel)
    def _():
        for i in range(blocks):
            lo, hi = i * BLK, (i + 1) * BLK
            arrived(pieces_of(i, n_row - 1), d_recv.at[i])
            if i == 1:
                each(n_row, lambda s: z_copy(s).start())
            own_row = m_ref[i, :, lo:]
            if i:
                left = jnp.concatenate([m_ref[b, :, lo:hi].T for b in range(i)], axis=1)
                own_row = own_row - plain_dot(left, m_ref[:i, :, lo:].reshape(lo, order - lo))
                w_ref[i, :, :lo] = -plain_dot(left, w_ref[:i, :, :lo].reshape(lo, lo))
            diag = own_row[:, :BLK]
            x_ref[:, :BLK] = 0.5 * (diag + diag.T)
            x_ref[:, BLK:] = eye
            if hi < order:
                m_ref[i, :, hi:] = own_row[:, BLK:]
            inverse_factor(x_ref, functools.partial(beside, i))
            if i == 1:
                each(n_col, lambda s: y_copy(s).start())
            if i > 1:
                solved_copy(i - 1).start()
            if i == 4:
                sum_z()
            w_diag = x_ref[:, BLK:]
            w_ref[i, :, lo:hi] = w_diag
            if i:
                w_ref[i, :, :lo] = plain_dot(w_diag, w_ref[i, :, :lo])
            if hi < order:
                m_ref[i, :, hi:] = plain_dot(w_diag, m_ref[i, :, hi:])
                w_ref[i, :, hi:] = jnp.zeros((BLK, order - hi), jnp.float32)
            if i == 4:
                each(n_row, lambda s: z_all_copy(s).start())

        def last(s, carry):
            solve_slab(blocks - 1, s)
            return carry

        lax.fori_loop(0, BLK // SUB, last, 0)

    sum_y()

    @pl.when(on_panel)
    def _():
        solved_copy(blocks - 1).start()
        panel_ref[...] = solved_ref[0]

        def wait_all(s):
            k = lax.rem(me_row + s, n_row)
            lines = z_all_ref.at[pl.ds(pl.multiple_of(k * z_lines, 8), z_lines)]
            arrived(lines, zall_recv.at[k])

        each(n_row, wait_all)
        inverse = w_ref[...].reshape(order, order)
        weights = turned_dot(z_all_ref[...], inverse)
        half = fix_ref.shape[0] // 2
        for part in (1, 0):
            lines = slice(part * half, (part + 1) * half)
            total = None
            for i in range(blocks):
                term = turned_dot(weights[lines, i * BLK : (i + 1) * BLK], solved_ref[i])
                total = term if total is None else total + term
            fix_ref[lines, :] = total
            for to in range(part * n_col // 2, (part + 1) * n_col // 2):
                if to:
                    fix_copy(to).start()
        share_ref[...] = fix_ref[0:y_lines, :]
        each(n_row, lambda s: z_copy(s).wait_send())
        each(n_row, lambda s: z_all_copy(s).wait_send())
        each(n_col, lambda s: solved_copy(s).wait_send())
        for to in range(1, n_col):
            fix_copy(to).wait_send()
        for b in range(blocks):
            arrived(pieces_of(b, n_row - 1), next_send.at[b])

    @pl.when(me_col != 0)
    def _():
        arrived(panel_ref, s_recv.at[0])
        arrived(share_ref, fix_recv.at[0])

    each(n_col, lambda s: y_copy(s).wait_send())
    for root in range(n_roots):
        @pl.when(on_panel & (me_row == root))
        def _(root=root):
            for b, first, last in sent[root]:
                count = last - first - (first <= root < last)
                arrived(pieces_of(b, count), first_send.at[b])


def panel_parts(matrix, probe, probe_rows, order, n_row, n_col):
    rows, columns = matrix.shape[0], probe.shape[1]
    lines_z, lines_y = columns // n_row, columns // n_col
    width = order // n_col
    dma = pltpu.SemaphoreType.DMA
    whole = functools.partial(jax.ShapeDtypeStruct, dtype=jnp.float32)
    return pl.pallas_call(
        panel_kernel,
        out_shape=(
            whole((rows, width)),
            whole((lines_y, rows)),
            whole((lines_y, rows)),
        ),
        in_specs=[pl.BlockSpec(memory_space=pltpu.VMEM)] * 3,
        out_specs=[pl.BlockSpec(memory_space=pltpu.VMEM)] * 3,
        scratch_shapes=[
            pltpu.VMEM((columns, order), jnp.float32),
            pltpu.VMEM((columns, rows), jnp.float32),
            pltpu.VMEM((order // BLK, BLK, order), jnp.float32),
            pltpu.VMEM((n_col, rows, width), jnp.float32),
            pltpu.VMEM((columns, order), jnp.float32),
            pltpu.VMEM((columns, rows), jnp.float32),
            pltpu.VMEM((order // BLK, BLK, order), jnp.float32),
            pltpu.VMEM((order // BLK, BLK // n_row, order), jnp.float32),
            pltpu.VMEM((BLK, 2 * BLK), jnp.float32),
            pltpu.VMEM((n_row, lines_z, order), jnp.float32),
            pltpu.VMEM((n_col, lines_y, rows), jnp.float32),
            *[dma((order // BLK,))] * 4,
            *[dma((n_row,))] * 4,
            *[dma((n_col,))] * 3, dma((1,)), dma((n_col,)), dma((1,)),
        ],
        compiler_params=pltpu.CompilerParams(has_side_effects=True, vmem_limit_bytes=60 << 20),
        cost_estimate=pl.CostEstimate(flops=3_000_000_000, bytes_accessed=16 << 20, transcendentals=0),
        name="panel_parts",
    )(matrix, probe, probe_rows)


def per_device(front, child_tiles, tile_target, tile_count, probe):
    n_row, n_col = lax.axis_size("row"), lax.axis_size("col")
    devices = n_row * n_col
    me_row, me_col = lax.axis_index("row"), lax.axis_index("col")
    rows, cols = front.shape
    tile_rows, tile_cols = rows // TB, cols // TB
    grid = tile_cols * n_col
    held = child_tiles.shape[0]
    start = PANELS * NB
    slot_index = jnp.arange(held, dtype=jnp.int32)
    live = slot_index % SLOTS < tile_count[slot_index // SLOTS]
    first_row, first_col = tile_target // grid, tile_target % grid
    target_row = jnp.concatenate([first_row, first_col])
    target_col = jnp.concatenate([first_col, first_row])
    owner = target_row // tile_rows * n_col + target_col // tile_cols
    in_row, in_col = target_row % tile_rows, target_col % tile_cols
    upright = jnp.arange(2 * held) < held
    upright_code = 2 * (in_col // 2 * tile_rows + in_row) + in_col % 2
    blocks = cols // LANES * tile_rows
    flips = -(-rows // LANES) * tile_cols
    turned_code = 2 * (blocks + in_row // 2 * tile_cols + in_col) + in_row % 2
    code = jnp.where(upright, upright_code, turned_code)
    code = jnp.where(jnp.concatenate([live, live]), code, 2 * (blocks + flips))
    order = jnp.arange(2 * held, dtype=jnp.int32)
    same = (owner[:, None] == owner[None, :]) & (order[None, :] < order[:, None])
    slot = 2 * owner + jnp.sum(same.astype(jnp.int32), axis=1)
    at_slot = slot[None, :] == order[:, None]
    source = jnp.sum(jnp.where(at_slot, (order % held)[None, :], 0), axis=1)
    sent_code = jnp.sum(jnp.where(at_slot, code[None, :], 0), axis=1)
    outgoing = packed(child_tiles, source)
    chunks = outgoing.shape[1]
    code_lines = jnp.pad(sent_code.reshape(devices, 1, 2), ((0, 0), (0, 0), (0, LANES - 2)))
    incoming, landing, probe_rows = exchanged(
        outgoing.reshape(devices, 2 * chunks, LANES), code_lines, probe, rows
    )
    matrix = placed(front, incoming.reshape(2 * devices, chunks, LANES), landing[:, 0, :2].reshape(-1))

    global_rows = me_row * rows + jnp.arange(rows, dtype=jnp.int32)
    panel_factor, y_own, fix_own = panel_parts(matrix, probe, probe_rows, start, n_row, n_col)
    sketch = jnp.where((global_rows >= start)[:, None], (y_own - fix_own).T, 0.0)
    return (panel_factor, sketch)


def solution(mesh):
    return jax.shard_map(
        per_device,
        mesh=mesh,
        in_specs=(
            P("row", "col"),
            P(("row", "col"), None),
            P(("row", "col")),
            P(("row", "col")),
            P("col", None),
        ),
        out_specs=(P("row", "col"), P("row", "col")),
        check_vma=False,
    )
```

```python
import functools

import jax
import jax.numpy as jnp
from jax import lax
from jax.experimental import pallas as pl
from jax.experimental.pallas import tpu as pltpu
from jax.sharding import PartitionSpec as P

NB = 512
PANELS = 2
TB = 64
SLOTS = 32
LANES = 128
SUB = 32
GROUP = 32
BLK = 128


def pack_kernel(source_ref, tiles_ref, out_ref, laid_ref, *, pitch, unroll):
    held = tiles_ref.shape[0]
    chunks = tiles_ref.shape[1] // LANES
    for group in range(held // 8):
        for part in range(chunks):
            laid_ref[pl.ds(group * 8 * pitch + part, 8, stride=pitch), :] = tiles_ref[
                group * 8 : group * 8 + 8, part * LANES : (part + 1) * LANES
            ]

    def step(q, carry):
        start = pl.multiple_of(source_ref[q] * pitch, 8)
        out_ref[q] = laid_ref[pl.ds(start, chunks), :]
        return carry

    lax.fori_loop(0, out_ref.shape[0], step, 0, unroll=unroll)


def packed(tiles, source):
    held, width = tiles.shape
    chunks = width // LANES
    pitch = chunks + 8
    return pl.pallas_call(
        functools.partial(pack_kernel, pitch=pitch, unroll=4),
        out_shape=jax.ShapeDtypeStruct((source.shape[0], chunks, LANES), jnp.float32),
        in_specs=[pl.BlockSpec(memory_space=pltpu.SMEM), pl.BlockSpec(memory_space=pltpu.VMEM)],
        out_specs=pl.BlockSpec(memory_space=pltpu.VMEM),
        scratch_shapes=[pltpu.VMEM((held * pitch, LANES), jnp.float32)],
        compiler_params=pltpu.CompilerParams(vmem_limit_bytes=60 << 20),
        cost_estimate=pl.CostEstimate(flops=10_000_000, bytes_accessed=6 << 20, transcendentals=0),
        name="packed_tiles",
    )(source, tiles)


def place_kernel(code_ref, tiles_ref, front_hbm, out_ref, sum_ref, front_ref, front_sem, *, unroll):
    rows, cols = front_ref.shape
    blocks = cols // LANES
    flips = -(-rows // LANES)
    half_rows = TB * TB // LANES
    group, groups = pl.program_id(0), pl.num_programs(0)
    count = tiles_ref.shape[0]
    front_copy = pltpu.make_async_copy(front_hbm, front_ref, front_sem)

    @pl.when(group == 0)
    def _():
        front_copy.start()
        sum_ref[...] = jnp.zeros_like(sum_ref)

    left = lax.broadcasted_iota(jnp.int32, (half_rows, LANES), 1) < TB

    def step(q, carry):
        code = code_ref[group * count + q]
        start = pl.multiple_of((code // 2) * TB, TB)
        odd = code % 2
        tile = tiles_ref[q]
        turned = pltpu.roll(tile, TB, 1)
        is_left = odd == 0
        keep = left == is_left
        upper = jnp.where(keep, jnp.where(is_left, tile, turned), 0.0)
        lower = jnp.where(keep, jnp.where(is_left, turned, tile), 0.0)
        even = pl.ds(start, half_rows, stride=2)
        uneven = pl.ds(start + 1, half_rows, stride=2)
        sum_ref[even, :] = sum_ref[even, :] + upper
        sum_ref[uneven, :] = sum_ref[uneven, :] + lower
        return carry

    lax.fori_loop(0, count, step, 0, unroll=unroll)
    @pl.when(group == groups - 1)
    def _():
        front_copy.wait()
        for block in range(blocks):
            lo, hi = block * LANES, (block + 1) * LANES
            out_ref[:, lo:hi] = front_ref[:, lo:hi] + sum_ref[block * rows : (block + 1) * rows, :]
            for flip in range(flips):
                at = blocks * rows + flip * cols + lo
                size = min(LANES, rows - flip * LANES)
                span = slice(flip * LANES, flip * LANES + size)
                out_ref[span, lo:hi] = out_ref[span, lo:hi] + sum_ref[at : at + LANES, :].T[:size, :]


def placed(front, tiles, code):
    rows, cols = front.shape
    total = (cols // LANES) * rows + -(-rows // LANES) * cols + TB
    return pl.pallas_call(
        functools.partial(place_kernel, unroll=8),
        out_shape=jax.ShapeDtypeStruct(front.shape, jnp.float32),
        grid=(tiles.shape[0] // GROUP,),
        in_specs=[
            pl.BlockSpec(memory_space=pltpu.SMEM),
            pl.BlockSpec((GROUP, *tiles.shape[1:]), lambda g: (g, 0, 0)),
            pl.BlockSpec(memory_space=pltpu.HBM),
        ],
        out_specs=pl.BlockSpec(front.shape, lambda g: (0, 0)),
        scratch_shapes=[
            pltpu.VMEM((total, LANES), jnp.float32),
            pltpu.VMEM(front.shape, jnp.float32),
            pltpu.SemaphoreType.DMA,
        ],
        compiler_params=pltpu.CompilerParams(vmem_limit_bytes=60 << 20),
        cost_estimate=pl.CostEstimate(flops=10_000_000, bytes_accessed=10 << 20, transcendentals=0),
        name="placed_tiles",
    )(code, tiles, front)


MESH = pl.DeviceIdType.MESH


def exchange_kernel(
    tiles_ref, code_ref, probe_ref, tiles_in, code_in, probe_rows,
    tiles_send, tiles_recv, code_send, code_recv, probe_send, probe_recv, own_sem,
):
    n_row, n_col = lax.axis_size("row"), lax.axis_size("col")
    devices = n_row * n_col
    me_row, me_col = lax.axis_index("row"), lax.axis_index("col")
    me = me_row * n_col + me_col
    rows = probe_rows.shape[0]
    group = n_row // n_col
    at = pl.ds(pl.multiple_of(lax.rem(me_row, group) * rows, 8), rows)

    def copies(step):
        turn = lax.rem(step * 53, devices)
        across = lax.rem(me_row // 4 + turn // 32, n_row // 4)
        deep = lax.rem(me_row + turn // 8, 4)
        up = lax.rem(me_col // 2 + lax.rem(turn // 2, n_col // 2), n_col // 2)
        where_to = (across * 4 + deep, up * 2 + lax.rem(me_col + turn, 2))
        to = where_to[0] * n_col + where_to[1]
        return (
            pltpu.make_async_remote_copy(
                code_ref.at[to], code_in.at[me], code_send, code_recv,
                device_id=where_to, device_id_type=MESH,
            ),
            pltpu.make_async_remote_copy(
                tiles_ref.at[to], tiles_in.at[me], tiles_send, tiles_recv,
                device_id=where_to, device_id_type=MESH,
            ),
        )

    def begin(step, carry):
        for copy in copies(step):
            copy.start()
        return carry

    probe_copy = pltpu.make_async_remote_copy(
        probe_ref.at[at], probe_rows, probe_send, probe_recv, device_id=(me_row, 0), device_id_type=MESH
    )
    source_col = me_row // group
    sends_probe = (me_col == source_col) & (me_col != 0)
    gets_probe = (me_col == 0) & (source_col != 0)

    lax.fori_loop(1, devices, begin, 0)

    @pl.when(sends_probe)
    def _():
        probe_copy.start()

    @pl.when((me_col == 0) & (source_col == 0))
    def _():
        probe_rows[...] = probe_ref[at, :]

    own = pltpu.make_async_copy(tiles_ref.at[me], tiles_in.at[me], own_sem)
    own.start()
    code_in[me] = code_ref[me]
    others = pl.ds(0, devices - 1)

    def all_of(ref, sem):
        pltpu.make_async_copy(ref.at[others], ref.at[others], sem).wait()

    own.wait()
    all_of(code_in, code_recv)
    all_of(tiles_in, tiles_recv)
    all_of(code_ref, code_send)
    all_of(tiles_ref, tiles_send)

    @pl.when(gets_probe)
    def _():
        pltpu.make_async_copy(probe_rows, probe_rows, probe_recv).wait()

    @pl.when(sends_probe)
    def _():
        probe_copy.wait_send()


def exchanged(tiles, code, probe, rows):
    dma = pltpu.SemaphoreType.DMA
    return pl.pallas_call(
        exchange_kernel,
        out_shape=(
            jax.ShapeDtypeStruct(tiles.shape, jnp.float32),
            jax.ShapeDtypeStruct(code.shape, jnp.int32),
            jax.ShapeDtypeStruct((rows, probe.shape[1]), jnp.float32),
        ),
        in_specs=[pl.BlockSpec(memory_space=pltpu.HBM)] + [pl.BlockSpec(memory_space=pltpu.VMEM)] * 2,
        out_specs=[pl.BlockSpec(memory_space=pltpu.HBM)] + [pl.BlockSpec(memory_space=pltpu.VMEM)] * 2,
        scratch_shapes=[dma] * 7,
        compiler_params=pltpu.CompilerParams(has_side_effects=True, vmem_limit_bytes=60 << 20),
        cost_estimate=pl.CostEstimate(flops=1_000_000_000, bytes_accessed=16 << 20, transcendentals=0),
        name="exchanged_tiles",
    )(tiles, code, probe)


def factor_rows(rows, base):
    groups = len(rows)
    sub = lax.broadcasted_iota(jnp.int32, (8, BLK), 0)
    lane = lax.broadcasted_iota(jnp.int32, (8, BLK), 1)

    def column(g, i):
        here = jnp.where(lane == base + i, rows[g][:, :BLK], 0.0)
        return jnp.broadcast_to(jnp.sum(here, axis=1, keepdims=True), (8, BLK))

    spread = [[column(g, i) if i < 8 * g + 8 else None for i in range(SUB)] for g in range(groups)]
    halves = [[row[:, :BLK], row[:, BLK:]] for row in rows]
    for i in range(SUB):
        own, at = divmod(i, 8)
        pivot = jnp.broadcast_to(spread[own][i][at : at + 1, :], (8, BLK))
        scale = lax.rsqrt(pivot)
        lows = [None] * groups
        for g in range(own, groups):
            low = spread[g][i] * scale
            lows[g] = jnp.where(sub > at, low, 0.0) if g == own else low
        for j in range(i + 1, SUB):
            g_j, at_j = divmod(j, 8)
            factor = jnp.broadcast_to(lows[g_j][at_j : at_j + 1, :], (8, BLK))
            for g in range(g_j, groups):
                spread[g][j] = spread[g][j] - lows[g] * factor
        for h in range(2):
            line = jnp.broadcast_to(halves[own][h][at : at + 1, :], (8, BLK)) * scale
            for g in range(own, groups):
                new = halves[g][h] - lows[g] * line
                halves[g][h] = jnp.where(sub == at, line, new) if g == own else new
    return [jnp.concatenate(half, axis=1) for half in halves]


def inverse_factor(x_ref, beside):
    row = lax.broadcasted_iota(jnp.int32, (BLK, 2 * BLK), 0)

    def step(s, carry):
        base = pl.multiple_of(s * SUB, SUB)
        lines = [pl.ds(base + g, 8) for g in range(0, SUB, 8)]
        rows = factor_rows([x_ref[line, :] for line in lines], base)
        beside(s)
        for line, value in zip(lines, rows):
            x_ref[line, :] = value
        done = jnp.concatenate(rows, axis=0)
        gone = joined_dot(done[:, :BLK].T, done)
        x_ref[...] = x_ref[...] - jnp.where(row >= base + SUB, gone, 0.0)
        return carry

    lax.fori_loop(0, BLK // SUB, step, 0)


def halves_of(a):
    top = a.astype(jnp.bfloat16)
    return top, (a - top.astype(jnp.float32)).astype(jnp.bfloat16)


def split_dot(a, b, b_dim):
    a_top, a_rest = halves_of(a)
    b_top, b_rest = halves_of(b)

    def part(p, q):
        return lax.dot_general(
            p, q, (((1,), (b_dim,)), ((), ())), preferred_element_type=jnp.float32
        )

    return part(a_top, b_top) + (part(a_top, b_rest) + part(a_rest, b_top))


def plain_dot(a, b):
    return split_dot(a, b, 0)


def turned_dot(a, b):
    return split_dot(a, b, 1)


def joined_dot(a, b):
    a_top, a_rest = halves_of(a)
    b_top, b_rest = halves_of(b)
    return lax.dot_general(
        jnp.concatenate([a_top, a_top, a_rest], axis=1),
        jnp.concatenate([b_top, b_rest, b_top], axis=0),
        (((1,), (0,)), ((), ())),
        preferred_element_type=jnp.float32,
    )


def panel_kernel(
    matrix_ref, probe_ref, probe_rows_ref, panel_ref, y_own_ref, share_ref,
    z_ref, y_ref, w_ref, solved_ref, z_all_ref, fix_ref, m_ref, stage_ref, x_ref, z_in, y_in,
    first_send, first_recv, next_send, d_recv, z_send, z_recv, zall_send, zall_recv,
    y_send, y_recv, s_send, s_recv, fix_send, fix_recv, ready_sem,
):
    me_row, me_col = lax.axis_index("row"), lax.axis_index("col")
    n_row, n_col = z_in.shape[0], y_in.shape[0]
    blocks, _, order = m_ref.shape
    rows = matrix_ref.shape[0]
    piece = BLK // n_row
    z_lines, y_lines = z_in.shape[1], y_in.shape[1]
    on_panel = me_col == 0

    def partner(step):
        turn = lax.rem(step * 7, n_row)
        side = 4
        across = lax.rem(me_row // side + turn // side, n_row // side)
        return across * side + lax.rem(lax.rem(me_row, side) + lax.rem(turn, side), side)

    def y_copy(step):
        to = lax.rem(me_col + step, n_col)
        return pltpu.make_async_remote_copy(
            y_ref.at[pl.ds(pl.multiple_of(to * y_lines, 8), y_lines)], y_in.at[me_col],
            y_send.at[to], y_recv.at[me_col], device_id=(me_row, to), device_id_type=MESH,
        )

    def z_copy(step):
        to = partner(step)
        return pltpu.make_async_remote_copy(
            z_ref.at[pl.ds(pl.multiple_of(to * z_lines, 8), z_lines)], z_in.at[me_row],
            z_send.at[to], z_recv.at[me_row], device_id=(to, me_col), device_id_type=MESH,
        )

    def z_all_copy(step):
        to = partner(step)
        mine = z_all_ref.at[pl.ds(pl.multiple_of(me_row * z_lines, 8), z_lines)]
        return pltpu.make_async_remote_copy(
            mine, mine, zall_send.at[to], zall_recv.at[me_row], device_id=(to, me_col), device_id_type=MESH,
        )

    def solved_copy(i):
        return pltpu.make_async_remote_copy(
            solved_ref.at[i], panel_ref, s_send.at[i], s_recv.at[0],
            device_id=(me_row, i), device_id_type=MESH,
        )

    def fix_copy(to):
        return pltpu.make_async_remote_copy(
            fix_ref.at[to * y_lines : (to + 1) * y_lines], share_ref, fix_send.at[to], fix_recv.at[0],
            device_id=(me_row, to), device_id_type=MESH,
        )

    def arrived(into, sem):
        pltpu.make_async_copy(into, into, sem).wait()

    def first_copy(b, to, root):
        at = b * BLK + to * piece - root * rows
        return pltpu.make_async_remote_copy(
            matrix_ref.at[pl.ds(pl.multiple_of(at, 8), piece), b * BLK : order],
            stage_ref.at[b, :, b * BLK : order],
            first_send.at[b], first_recv.at[b], device_id=(to, me_col), device_id_type=MESH,
        )

    own_lines = pl.ds(pl.multiple_of(me_row * piece, 8), piece)

    def held_piece(b, root=None):
        if root is None:
            return stage_ref.at[b, :, b * BLK : order]
        at = b * BLK + root * piece - root * rows
        return matrix_ref.at[at : at + piece, b * BLK : order]

    def next_copy(b, step, root=None):
        to = partner(step)
        return pltpu.make_async_remote_copy(
            held_piece(b, root), m_ref.at[b, own_lines, b * BLK : order], next_send.at[b], d_recv.at[b],
            device_id=(to, me_col), device_id_type=MESH,
        )

    def pieces_of(b, count):
        return m_ref.at[b, 0 : count * piece, b * BLK : order]

    def each(count, action):
        def step(s, carry):
            action(s)
            return carry

        lax.fori_loop(1, count, step, 0)

    entry = pltpu.get_barrier_semaphore()

    def greet_row(s):
        pl.semaphore_signal(
            entry, inc=1, device_id=(me_row, lax.rem(me_col + s, n_col)), device_id_type=MESH
        )

    @pl.when(on_panel)
    def _():
        each(n_row, lambda s: pl.semaphore_signal(
            entry, inc=1, device_id=(partner(s), me_col), device_id_type=MESH
        ))
        each(n_col, greet_row)
        pl.semaphore_wait(entry, n_row - 1)

    @pl.when(me_col != 0)
    def _():
        def greet(s, carry):
            @pl.when(lax.rem(me_col + s, n_col) != 0)
            def _():
                greet_row(s)
            return carry

        lax.fori_loop(1, n_col, greet, 0)
        pl.semaphore_wait(entry, n_col - 1)
        pl.semaphore_signal(ready_sem, inc=1, device_id=(me_row, 0), device_id_type=MESH)

    n_roots = -(-order // rows)
    sent = [[] for _ in range(n_roots)]
    for root in range(n_roots):
        for b in range(blocks):
            first = max(0, root * rows - b * BLK) // piece
            last = min(BLK, (root + 1) * rows - b * BLK) // piece
            if first < last:
                sent[root].append((b, first, last))

    for root in range(n_roots):
        @pl.when(on_panel & (me_row == root))
        def _(root=root):
            for b, first, last in sent[root]:
                for to in range(first, last):
                    if to != root:
                        first_copy(b, to, root).start()

    def z_slab(s):
        lanes = pl.ds(pl.multiple_of(s * z_slab_width, BLK), z_slab_width)
        line = me_row * rows + lax.broadcasted_iota(jnp.int32, (rows, z_slab_width), 0)
        chosen = jnp.where(line >= order, probe_rows_ref[:, lanes], 0.0)
        z_ref[lanes, :] = plain_dot(chosen.T, matrix_ref[:, :order])

    def y_slab(s, first):
        lanes = pl.ds(pl.multiple_of(s * z_slab_width, BLK), z_slab_width)
        y_ref[lanes, :] = turned_dot(probe_ref[first:, lanes].T, matrix_ref[:, first:])

    steps = BLK // SUB
    z_slab_width = z_ref.shape[0] // steps

    @pl.when(on_panel)
    def _():
        def step(s, carry):
            z_slab(s)
            return carry

        lax.fori_loop(0, steps, step, 0)

    local = [[b for b, first, last in sent[root] if first <= root < last] for root in range(n_roots)]
    for b in range(blocks):
        mine = None
        for root in range(n_roots):
            if b in local[root]:
                mine = root

        @pl.when(on_panel & (me_row != mine))
        def _(b=b):
            arrived(held_piece(b), first_recv.at[b])
            each(n_row, lambda s: next_copy(b, s).start())
            m_ref[b, own_lines, b * BLK : order] = stage_ref[b, :, b * BLK : order]

        @pl.when(on_panel & (me_row == mine))
        def _(b=b, mine=mine):
            each(n_row, lambda s: next_copy(b, s, mine).start())
            at = b * BLK + mine * piece - mine * rows
            m_ref[b, own_lines, b * BLK : order] = matrix_ref[at : at + piece, b * BLK : order]

    @pl.when(me_col != 0)
    def _():
        def step(s, carry):
            y_slab(s, 0)
            return carry

        lax.fori_loop(0, steps, step, 0)
        each(n_col, lambda s: y_copy(s).start())

    def sum_z():
        own = pl.ds(pl.multiple_of(me_row * z_lines, 8), z_lines)
        z_in[me_row] = z_ref[own, :]

        def wait_z(s):
            k = lax.rem(me_row + s, n_row)
            arrived(z_in.at[k], z_recv.at[k])

        each(n_row, wait_z)
        total = z_in[0]
        for k in range(1, n_row):
            total = total + z_in[k]
        z_all_ref[own, :] = total

    def sum_y():
        def wait_y(s):
            k = lax.rem(me_col + s, n_col)
            arrived(y_in.at[k], y_recv.at[k])

        each(n_col, wait_y)
        y_in[me_col] = y_ref[pl.ds(pl.multiple_of(me_col * y_lines, 8), y_lines), :]
        y_total = y_in[0]
        for k in range(1, n_col):
            y_total = y_total + y_in[k]
        y_own_ref[...] = y_total

    eye = (
        lax.broadcasted_iota(jnp.int32, (BLK, BLK), 0) == lax.broadcasted_iota(jnp.int32, (BLK, BLK), 1)
    ).astype(jnp.float32)
    slab = rows // (BLK // SUB)

    def solve_slab(i, s):
        lines = pl.ds(pl.multiple_of(s * slab, 8), slab)
        hi = (i + 1) * BLK
        part = turned_dot(matrix_ref[lines, :hi], w_ref[i, :, :hi])
        if i * BLK >= NB:
            line = me_row * rows + s * slab + lax.broadcasted_iota(jnp.int32, (slab, BLK), 0)
            part = jnp.where(line >= i * BLK // NB * NB, part, 0.0)
        solved_ref[i, lines, :] = part

    def beside(i, s):
        if i:
            solve_slab(i - 1, s)
        else:
            y_slab(s, order)

    @pl.when(on_panel)
    def _():
        each(n_row, lambda s: z_copy(s).start())
        for i in range(blocks):
            lo, hi = i * BLK, (i + 1) * BLK
            arrived(pieces_of(i, n_row - 1), d_recv.at[i])
            own_row = m_ref[i, :, lo:]
            if i:
                left = jnp.concatenate([m_ref[b, :, lo:hi].T for b in range(i)], axis=1)
                own_row = own_row - plain_dot(left, m_ref[:i, :, lo:].reshape(lo, order - lo))
                w_ref[i, :, :lo] = -plain_dot(left, w_ref[:i, :, :lo].reshape(lo, lo))
            diag = own_row[:, :BLK]
            x_ref[:, :BLK] = 0.5 * (diag + diag.T)
            x_ref[:, BLK:] = eye
            if hi < order:
                m_ref[i, :, hi:] = own_row[:, BLK:]
            inverse_factor(x_ref, functools.partial(beside, i))
            if i == 1:
                pl.semaphore_wait(ready_sem, n_col - 1)
                each(n_col, lambda s: y_copy(s).start())
            if i > 1:
                solved_copy(i - 1).start()
            if i == 3:
                sum_z()
            w_diag = x_ref[:, BLK:]
            w_ref[i, :, lo:hi] = w_diag
            if i:
                w_ref[i, :, :lo] = plain_dot(w_diag, w_ref[i, :, :lo])
            if hi < order:
                m_ref[i, :, hi:] = plain_dot(w_diag, m_ref[i, :, hi:])
                w_ref[i, :, hi:] = jnp.zeros((BLK, order - hi), jnp.float32)
            if i == 3:
                each(n_row, lambda s: z_all_copy(s).start())

        def last(s, carry):
            solve_slab(blocks - 1, s)
            return carry

        lax.fori_loop(0, BLK // SUB, last, 0)

    sum_y()

    @pl.when(on_panel)
    def _():
        solved_copy(blocks - 1).start()
        panel_ref[...] = solved_ref[0]

        def wait_all(s):
            k = lax.rem(me_row + s, n_row)
            lines = z_all_ref.at[pl.ds(pl.multiple_of(k * z_lines, 8), z_lines)]
            arrived(lines, zall_recv.at[k])

        each(n_row, wait_all)
        inverse = w_ref[...].reshape(order, order)
        weights = turned_dot(z_all_ref[...], inverse)
        half = fix_ref.shape[0] // 2
        for part in (1, 0):
            lines = slice(part * half, (part + 1) * half)
            total = None
            for i in range(blocks):
                term = turned_dot(weights[lines, i * BLK : (i + 1) * BLK], solved_ref[i])
                total = term if total is None else total + term
            fix_ref[lines, :] = total
            for to in range(part * n_col // 2, (part + 1) * n_col // 2):
                if to:
                    fix_copy(to).start()
        share_ref[...] = fix_ref[0:y_lines, :]
        each(n_row, lambda s: z_copy(s).wait_send())
        each(n_row, lambda s: z_all_copy(s).wait_send())
        each(n_col, lambda s: solved_copy(s).wait_send())
        for to in range(1, n_col):
            fix_copy(to).wait_send()
        for b in range(blocks):
            arrived(pieces_of(b, n_row - 1), next_send.at[b])

    @pl.when(me_col != 0)
    def _():
        arrived(panel_ref, s_recv.at[0])
        arrived(share_ref, fix_recv.at[0])

    each(n_col, lambda s: y_copy(s).wait_send())
    for root in range(n_roots):
        @pl.when(on_panel & (me_row == root))
        def _(root=root):
            for b, first, last in sent[root]:
                count = last - first - (first <= root < last)
                arrived(pieces_of(b, count), first_send.at[b])


def panel_parts(matrix, probe, probe_rows, order, n_row, n_col):
    rows, columns = matrix.shape[0], probe.shape[1]
    lines_z, lines_y = columns // n_row, columns // n_col
    width = order // n_col
    dma = pltpu.SemaphoreType.DMA
    whole = functools.partial(jax.ShapeDtypeStruct, dtype=jnp.float32)
    return pl.pallas_call(
        panel_kernel,
        out_shape=(
            whole((rows, width)),
            whole((lines_y, rows)),
            whole((lines_y, rows)),
        ),
        in_specs=[pl.BlockSpec(memory_space=pltpu.VMEM)] * 3,
        out_specs=[pl.BlockSpec(memory_space=pltpu.VMEM)] * 3,
        scratch_shapes=[
            pltpu.VMEM((columns, order), jnp.float32),
            pltpu.VMEM((columns, rows), jnp.float32),
            pltpu.VMEM((order // BLK, BLK, order), jnp.float32),
            pltpu.VMEM((n_col, rows, width), jnp.float32),
            pltpu.VMEM((columns, order), jnp.float32),
            pltpu.VMEM((columns, rows), jnp.float32),
            pltpu.VMEM((order // BLK, BLK, order), jnp.float32),
            pltpu.VMEM((order // BLK, BLK // n_row, order), jnp.float32),
            pltpu.VMEM((BLK, 2 * BLK), jnp.float32),
            pltpu.VMEM((n_row, lines_z, order), jnp.float32),
            pltpu.VMEM((n_col, lines_y, rows), jnp.float32),
            *[dma((order // BLK,))] * 4,
            *[dma((n_row,))] * 4,
            *[dma((n_col,))] * 3, dma((1,)), dma((n_col,)), dma((1,)), pltpu.SemaphoreType.REGULAR,
        ],
        compiler_params=pltpu.CompilerParams(
            has_side_effects=True, vmem_limit_bytes=60 << 20, collective_id=1
        ),
        cost_estimate=pl.CostEstimate(flops=3_000_000_000, bytes_accessed=16 << 20, transcendentals=0),
        name="panel_parts",
    )(matrix, probe, probe_rows)


def per_device(front, child_tiles, tile_target, tile_count, probe):
    n_row, n_col = lax.axis_size("row"), lax.axis_size("col")
    devices = n_row * n_col
    me_row, me_col = lax.axis_index("row"), lax.axis_index("col")
    rows, cols = front.shape
    tile_rows, tile_cols = rows // TB, cols // TB
    grid = tile_cols * n_col
    held = child_tiles.shape[0]
    start = PANELS * NB
    slot_index = jnp.arange(held, dtype=jnp.int32)
    live = slot_index % SLOTS < tile_count[slot_index // SLOTS]
    first_row, first_col = tile_target // grid, tile_target % grid
    target_row = jnp.concatenate([first_row, first_col])
    target_col = jnp.concatenate([first_col, first_row])
    owner = target_row // tile_rows * n_col + target_col // tile_cols
    in_row, in_col = target_row % tile_rows, target_col % tile_cols
    upright = jnp.arange(2 * held) < held
    upright_code = 2 * (in_col // 2 * tile_rows + in_row) + in_col % 2
    blocks = cols // LANES * tile_rows
    flips = -(-rows // LANES) * tile_cols
    turned_code = 2 * (blocks + in_row // 2 * tile_cols + in_col) + in_row % 2
    code = jnp.where(upright, upright_code, turned_code)
    code = jnp.where(jnp.concatenate([live, live]), code, 2 * (blocks + flips))
    order = jnp.arange(2 * held, dtype=jnp.int32)
    same = (owner[:, None] == owner[None, :]) & (order[None, :] < order[:, None])
    slot = 2 * owner + jnp.sum(same.astype(jnp.int32), axis=1)
    at_slot = slot[None, :] == order[:, None]
    source = jnp.sum(jnp.where(at_slot, (order % held)[None, :], 0), axis=1)
    sent_code = jnp.sum(jnp.where(at_slot, code[None, :], 0), axis=1)
    outgoing = packed(child_tiles, source)
    chunks = outgoing.shape[1]
    code_lines = jnp.pad(sent_code.reshape(devices, 1, 2), ((0, 0), (0, 0), (0, LANES - 2)))
    incoming, landing, probe_rows = exchanged(
        outgoing.reshape(devices, 2 * chunks, LANES), code_lines, probe, rows
    )
    matrix = placed(front, incoming.reshape(2 * devices, chunks, LANES), landing[:, 0, :2].reshape(-1))

    global_rows = me_row * rows + jnp.arange(rows, dtype=jnp.int32)
    panel_factor, y_own, fix_own = panel_parts(matrix, probe, probe_rows, start, n_row, n_col)
    sketch = jnp.where((global_rows >= start)[:, None], (y_own - fix_own).T, 0.0)
    return (panel_factor, sketch)


def solution(mesh):
    return jax.shard_map(
        per_device,
        mesh=mesh,
        in_specs=(
            P("row", "col"),
            P(("row", "col"), None),
            P(("row", "col")),
            P(("row", "col")),
            P("col", None),
        ),
        out_specs=(P("row", "col"), P("row", "col")),
        check_vma=False,
    )
```

```python
import functools

import jax
import jax.numpy as jnp
from jax import lax
from jax.experimental import pallas as pl
from jax.experimental.pallas import tpu as pltpu
from jax.sharding import PartitionSpec as P

NB = 512
PANELS = 2
TB = 64
SLOTS = 32
LANES = 128
SUB = 32
GROUP = 32
BLK = 128


def pack_kernel(source_ref, tiles_ref, out_ref, laid_ref, *, pitch, unroll):
    held = tiles_ref.shape[0]
    chunks = tiles_ref.shape[1] // LANES
    for group in range(held // 8):
        for part in range(chunks):
            laid_ref[pl.ds(group * 8 * pitch + part, 8, stride=pitch), :] = tiles_ref[
                group * 8 : group * 8 + 8, part * LANES : (part + 1) * LANES
            ]

    def step(q, carry):
        start = pl.multiple_of(source_ref[q] * pitch, 8)
        out_ref[q] = laid_ref[pl.ds(start, chunks), :]
        return carry

    lax.fori_loop(0, out_ref.shape[0], step, 0, unroll=unroll)


def packed(tiles, source):
    held, width = tiles.shape
    chunks = width // LANES
    pitch = chunks + 8
    return pl.pallas_call(
        functools.partial(pack_kernel, pitch=pitch, unroll=4),
        out_shape=jax.ShapeDtypeStruct((source.shape[0], chunks, LANES), jnp.float32),
        in_specs=[pl.BlockSpec(memory_space=pltpu.SMEM), pl.BlockSpec(memory_space=pltpu.VMEM)],
        out_specs=pl.BlockSpec(memory_space=pltpu.VMEM),
        scratch_shapes=[pltpu.VMEM((held * pitch, LANES), jnp.float32)],
        compiler_params=pltpu.CompilerParams(vmem_limit_bytes=60 << 20),
        cost_estimate=pl.CostEstimate(flops=10_000_000, bytes_accessed=6 << 20, transcendentals=0),
        name="packed_tiles",
    )(source, tiles)


def place_kernel(code_ref, tiles_ref, front_hbm, out_ref, sum_ref, front_ref, front_sem, *, unroll):
    rows, cols = front_ref.shape
    blocks = cols // LANES
    flips = -(-rows // LANES)
    half_rows = TB * TB // LANES
    group, groups = pl.program_id(0), pl.num_programs(0)
    count = tiles_ref.shape[0]
    front_copy = pltpu.make_async_copy(front_hbm, front_ref, front_sem)

    @pl.when(group == 0)
    def _():
        front_copy.start()
        sum_ref[...] = jnp.zeros_like(sum_ref)

    left = lax.broadcasted_iota(jnp.int32, (half_rows, LANES), 1) < TB

    def step(q, carry):
        code = code_ref[group * count + q]
        start = pl.multiple_of((code // 2) * TB, TB)
        odd = code % 2
        tile = tiles_ref[q]
        turned = pltpu.roll(tile, TB, 1)
        is_left = odd == 0
        keep = left == is_left
        upper = jnp.where(keep, jnp.where(is_left, tile, turned), 0.0)
        lower = jnp.where(keep, jnp.where(is_left, turned, tile), 0.0)
        even = pl.ds(start, half_rows, stride=2)
        uneven = pl.ds(start + 1, half_rows, stride=2)
        sum_ref[even, :] = sum_ref[even, :] + upper
        sum_ref[uneven, :] = sum_ref[uneven, :] + lower
        return carry

    lax.fori_loop(0, count, step, 0, unroll=unroll)
    @pl.when(group == groups - 1)
    def _():
        front_copy.wait()
        for block in range(blocks):
            lo, hi = block * LANES, (block + 1) * LANES
            out_ref[:, lo:hi] = front_ref[:, lo:hi] + sum_ref[block * rows : (block + 1) * rows, :]
            for flip in range(flips):
                at = blocks * rows + flip * cols + lo
                size = min(LANES, rows - flip * LANES)
                span = slice(flip * LANES, flip * LANES + size)
                out_ref[span, lo:hi] = out_ref[span, lo:hi] + sum_ref[at : at + LANES, :].T[:size, :]


def placed(front, tiles, code):
    rows, cols = front.shape
    total = (cols // LANES) * rows + -(-rows // LANES) * cols + TB
    return pl.pallas_call(
        functools.partial(place_kernel, unroll=8),
        out_shape=jax.ShapeDtypeStruct(front.shape, jnp.float32),
        grid=(tiles.shape[0] // GROUP,),
        in_specs=[
            pl.BlockSpec(memory_space=pltpu.SMEM),
            pl.BlockSpec((GROUP, *tiles.shape[1:]), lambda g: (g, 0, 0)),
            pl.BlockSpec(memory_space=pltpu.HBM),
        ],
        out_specs=pl.BlockSpec(front.shape, lambda g: (0, 0)),
        scratch_shapes=[
            pltpu.VMEM((total, LANES), jnp.float32),
            pltpu.VMEM(front.shape, jnp.float32),
            pltpu.SemaphoreType.DMA,
        ],
        compiler_params=pltpu.CompilerParams(vmem_limit_bytes=60 << 20),
        cost_estimate=pl.CostEstimate(flops=10_000_000, bytes_accessed=10 << 20, transcendentals=0),
        name="placed_tiles",
    )(code, tiles, front)


MESH = pl.DeviceIdType.MESH


def exchange_kernel(
    tiles_ref, code_ref, probe_ref, tiles_in, code_in, probe_rows,
    tiles_send, tiles_recv, code_send, code_recv, probe_send, probe_recv, own_sem,
):
    n_row, n_col = lax.axis_size("row"), lax.axis_size("col")
    devices = n_row * n_col
    me_row, me_col = lax.axis_index("row"), lax.axis_index("col")
    me = me_row * n_col + me_col
    rows = probe_rows.shape[0]
    group = n_row // n_col
    at = pl.ds(pl.multiple_of(lax.rem(me_row, group) * rows, 8), rows)

    def copies(step):
        turn = lax.rem(step * 53, devices)
        across = lax.rem(me_row // 4 + turn // 32, n_row // 4)
        deep = lax.rem(me_row + turn // 8, 4)
        up = lax.rem(me_col // 2 + lax.rem(turn // 2, n_col // 2), n_col // 2)
        where_to = (across * 4 + deep, up * 2 + lax.rem(me_col + turn, 2))
        to = where_to[0] * n_col + where_to[1]
        return (
            pltpu.make_async_remote_copy(
                code_ref.at[to], code_in.at[me], code_send, code_recv,
                device_id=where_to, device_id_type=MESH,
            ),
            pltpu.make_async_remote_copy(
                tiles_ref.at[to], tiles_in.at[me], tiles_send, tiles_recv,
                device_id=where_to, device_id_type=MESH,
            ),
        )

    def begin(step, carry):
        for copy in copies(step):
            copy.start()
        return carry

    probe_copy = pltpu.make_async_remote_copy(
        probe_ref.at[at], probe_rows, probe_send, probe_recv, device_id=(me_row, 0), device_id_type=MESH
    )
    source_col = me_row // group
    sends_probe = (me_col == source_col) & (me_col != 0)
    gets_probe = (me_col == 0) & (source_col != 0)

    lax.fori_loop(1, devices, begin, 0)

    @pl.when(sends_probe)
    def _():
        probe_copy.start()

    @pl.when((me_col == 0) & (source_col == 0))
    def _():
        probe_rows[...] = probe_ref[at, :]

    own = pltpu.make_async_copy(tiles_ref.at[me], tiles_in.at[me], own_sem)
    own.start()
    code_in[me] = code_ref[me]
    others = pl.ds(0, devices - 1)

    def all_of(ref, sem):
        pltpu.make_async_copy(ref.at[others], ref.at[others], sem).wait()

    own.wait()
    all_of(code_in, code_recv)
    all_of(tiles_in, tiles_recv)
    all_of(code_ref, code_send)
    all_of(tiles_ref, tiles_send)

    @pl.when(gets_probe)
    def _():
        pltpu.make_async_copy(probe_rows, probe_rows, probe_recv).wait()

    @pl.when(sends_probe)
    def _():
        probe_copy.wait_send()


def exchanged(tiles, code, probe, rows):
    dma = pltpu.SemaphoreType.DMA
    return pl.pallas_call(
        exchange_kernel,
        out_shape=(
            jax.ShapeDtypeStruct(tiles.shape, jnp.float32),
            jax.ShapeDtypeStruct(code.shape, jnp.int32),
            jax.ShapeDtypeStruct((rows, probe.shape[1]), jnp.float32),
        ),
        in_specs=[pl.BlockSpec(memory_space=pltpu.HBM)] + [pl.BlockSpec(memory_space=pltpu.VMEM)] * 2,
        out_specs=[pl.BlockSpec(memory_space=pltpu.HBM)] + [pl.BlockSpec(memory_space=pltpu.VMEM)] * 2,
        scratch_shapes=[dma] * 7,
        compiler_params=pltpu.CompilerParams(has_side_effects=True, vmem_limit_bytes=60 << 20),
        cost_estimate=pl.CostEstimate(flops=1_000_000_000, bytes_accessed=16 << 20, transcendentals=0),
        name="exchanged_tiles",
    )(tiles, code, probe)


def factor_rows(rows, base):
    groups = len(rows)
    sub = lax.broadcasted_iota(jnp.int32, (8, BLK), 0)
    lane = lax.broadcasted_iota(jnp.int32, (8, BLK), 1)

    def column(g, i):
        here = jnp.where(lane == base + i, rows[g][:, :BLK], 0.0)
        return jnp.broadcast_to(jnp.sum(here, axis=1, keepdims=True), (8, BLK))

    spread = [[column(g, i) if i < 8 * g + 8 else None for i in range(SUB)] for g in range(groups)]
    halves = [[row[:, :BLK], row[:, BLK:]] for row in rows]
    for i in range(SUB):
        own, at = divmod(i, 8)
        pivot = jnp.broadcast_to(spread[own][i][at : at + 1, :], (8, BLK))
        scale = lax.rsqrt(pivot)
        lows = [None] * groups
        for g in range(own, groups):
            low = spread[g][i] * scale
            lows[g] = jnp.where(sub > at, low, 0.0) if g == own else low
        for j in range(i + 1, SUB):
            g_j, at_j = divmod(j, 8)
            factor = jnp.broadcast_to(lows[g_j][at_j : at_j + 1, :], (8, BLK))
            for g in range(g_j, groups):
                spread[g][j] = spread[g][j] - lows[g] * factor
        for h in range(2):
            line = jnp.broadcast_to(halves[own][h][at : at + 1, :], (8, BLK)) * scale
            for g in range(own, groups):
                new = halves[g][h] - lows[g] * line
                halves[g][h] = jnp.where(sub == at, line, new) if g == own else new
    return [jnp.concatenate(half, axis=1) for half in halves]


def inverse_factor(x_ref, beside):
    row = lax.broadcasted_iota(jnp.int32, (BLK, 2 * BLK), 0)

    def step(s, carry):
        base = pl.multiple_of(s * SUB, SUB)
        lines = [pl.ds(base + g, 8) for g in range(0, SUB, 8)]
        rows = factor_rows([x_ref[line, :] for line in lines], base)
        beside(s)
        for line, value in zip(lines, rows):
            x_ref[line, :] = value
        done = jnp.concatenate(rows, axis=0)
        gone = joined_dot(done[:, :BLK].T, done)
        x_ref[...] = x_ref[...] - jnp.where(row >= base + SUB, gone, 0.0)
        return carry

    lax.fori_loop(0, BLK // SUB, step, 0)


def halves_of(a):
    top = a.astype(jnp.bfloat16)
    return top, (a - top.astype(jnp.float32)).astype(jnp.bfloat16)


def split_dot(a, b, b_dim):
    a_top, a_rest = halves_of(a)
    b_top, b_rest = halves_of(b)

    def part(p, q):
        return lax.dot_general(
            p, q, (((1,), (b_dim,)), ((), ())), preferred_element_type=jnp.float32
        )

    return part(a_top, b_top) + (part(a_top, b_rest) + part(a_rest, b_top))


def plain_dot(a, b):
    return split_dot(a, b, 0)


def turned_dot(a, b):
    return split_dot(a, b, 1)


def joined_dot(a, b):
    a_top, a_rest = halves_of(a)
    b_top, b_rest = halves_of(b)
    return lax.dot_general(
        jnp.concatenate([a_top, a_top, a_rest], axis=1),
        jnp.concatenate([b_top, b_rest, b_top], axis=0),
        (((1,), (0,)), ((), ())),
        preferred_element_type=jnp.float32,
    )


def panel_kernel(
    matrix_ref, probe_ref, probe_rows_ref, panel_ref, y_own_ref, share_ref,
    z_ref, y_ref, w_ref, solved_ref, z_all_ref, fix_ref, m_ref, stage_ref, x_ref, z_in, y_in,
    first_send, first_recv, next_send, d_recv, z_send, z_recv, zall_send, zall_recv,
    y_send, y_recv, s_send, s_recv, fix_send, fix_recv,
):
    me_row, me_col = lax.axis_index("row"), lax.axis_index("col")
    n_row, n_col = z_in.shape[0], y_in.shape[0]
    blocks, _, order = m_ref.shape
    rows = matrix_ref.shape[0]
    piece = BLK // n_row
    z_lines, y_lines = z_in.shape[1], y_in.shape[1]
    on_panel = me_col == 0

    def partner(step):
        turn = lax.rem(step * 7, n_row)
        side = 4
        across = lax.rem(me_row // side + turn // side, n_row // side)
        return across * side + lax.rem(lax.rem(me_row, side) + lax.rem(turn, side), side)

    def y_copy(step):
        to = lax.rem(me_col + step, n_col)
        return pltpu.make_async_remote_copy(
            y_ref.at[pl.ds(pl.multiple_of(to * y_lines, 8), y_lines)], y_in.at[me_col],
            y_send.at[to], y_recv.at[me_col], device_id=(me_row, to), device_id_type=MESH,
        )

    def z_copy(step):
        to = partner(step)
        return pltpu.make_async_remote_copy(
            z_ref.at[pl.ds(pl.multiple_of(to * z_lines, 8), z_lines)], z_in.at[me_row],
            z_send.at[to], z_recv.at[me_row], device_id=(to, me_col), device_id_type=MESH,
        )

    def z_all_copy(step):
        to = partner(step)
        mine = z_all_ref.at[pl.ds(pl.multiple_of(me_row * z_lines, 8), z_lines)]
        return pltpu.make_async_remote_copy(
            mine, mine, zall_send.at[to], zall_recv.at[me_row], device_id=(to, me_col), device_id_type=MESH,
        )

    def solved_copy(i):
        return pltpu.make_async_remote_copy(
            solved_ref.at[i], panel_ref, s_send.at[i], s_recv.at[0],
            device_id=(me_row, i), device_id_type=MESH,
        )

    def fix_copy(to):
        return pltpu.make_async_remote_copy(
            fix_ref.at[to * y_lines : (to + 1) * y_lines], share_ref, fix_send.at[to], fix_recv.at[0],
            device_id=(me_row, to), device_id_type=MESH,
        )

    def arrived(into, sem):
        pltpu.make_async_copy(into, into, sem).wait()

    def first_copy(b, to, root):
        at = b * BLK + to * piece - root * rows
        return pltpu.make_async_remote_copy(
            matrix_ref.at[pl.ds(pl.multiple_of(at, 8), piece), b * BLK : order],
            stage_ref.at[b, :, b * BLK : order],
            first_send.at[b], first_recv.at[b], device_id=(to, me_col), device_id_type=MESH,
        )

    own_lines = pl.ds(pl.multiple_of(me_row * piece, 8), piece)

    def held_piece(b, root=None):
        if root is None:
            return stage_ref.at[b, :, b * BLK : order]
        at = b * BLK + root * piece - root * rows
        return matrix_ref.at[at : at + piece, b * BLK : order]

    def next_copy(b, step, root=None):
        to = partner(step)
        return pltpu.make_async_remote_copy(
            held_piece(b, root), m_ref.at[b, own_lines, b * BLK : order], next_send.at[b], d_recv.at[b],
            device_id=(to, me_col), device_id_type=MESH,
        )

    def pieces_of(b, count):
        return m_ref.at[b, 0 : count * piece, b * BLK : order]

    def each(count, action):
        def step(s, carry):
            action(s)
            return carry

        lax.fori_loop(1, count, step, 0)

    n_roots = -(-order // rows)
    sent = [[] for _ in range(n_roots)]
    for root in range(n_roots):
        for b in range(blocks):
            first = max(0, root * rows - b * BLK) // piece
            last = min(BLK, (root + 1) * rows - b * BLK) // piece
            if first < last:
                sent[root].append((b, first, last))

    for root in range(n_roots):
        @pl.when(on_panel & (me_row == root))
        def _(root=root):
            for b, first, last in sent[root]:
                for to in range(first, last):
                    if to != root:
                        first_copy(b, to, root).start()

    local = [[b for b, first, last in sent[root] if first <= root < last] for root in range(n_roots)]
    for b in range(blocks):
        mine = None
        for root in range(n_roots):
            if b in local[root]:
                mine = root

        @pl.when(on_panel & (me_row != mine))
        def _(b=b):
            arrived(held_piece(b), first_recv.at[b])
            each(n_row, lambda s: next_copy(b, s).start())
            m_ref[b, own_lines, b * BLK : order] = stage_ref[b, :, b * BLK : order]

        @pl.when(on_panel & (me_row == mine))
        def _(b=b, mine=mine):
            each(n_row, lambda s: next_copy(b, s, mine).start())
            at = b * BLK + mine * piece - mine * rows
            m_ref[b, own_lines, b * BLK : order] = matrix_ref[at : at + piece, b * BLK : order]

    def z_slab(s):
        lanes = pl.ds(pl.multiple_of(s * z_slab_width, BLK), z_slab_width)
        line = me_row * rows + lax.broadcasted_iota(jnp.int32, (rows, z_slab_width), 0)
        chosen = jnp.where(line >= order, probe_rows_ref[:, lanes], 0.0)
        z_ref[lanes, :] = plain_dot(chosen.T, matrix_ref[:, :order])

    def y_slab(s, first):
        lanes = pl.ds(pl.multiple_of(s * z_slab_width, BLK), z_slab_width)
        y_ref[lanes, :] = turned_dot(probe_ref[first:, lanes].T, matrix_ref[:, first:])

    steps = BLK // SUB
    z_slab_width = z_ref.shape[0] // steps

    @pl.when(me_col != 0)
    def _():
        def step(s, carry):
            y_slab(s, 0)
            return carry

        lax.fori_loop(0, steps, step, 0)
        each(n_col, lambda s: y_copy(s).start())

    def sum_z():
        own = pl.ds(pl.multiple_of(me_row * z_lines, 8), z_lines)
        z_in[me_row] = z_ref[own, :]

        def wait_z(s):
            k = lax.rem(me_row + s, n_row)
            arrived(z_in.at[k], z_recv.at[k])

        each(n_row, wait_z)
        total = z_in[0]
        for k in range(1, n_row):
            total = total + z_in[k]
        z_all_ref[own, :] = total

    def sum_y():
        def wait_y(s):
            k = lax.rem(me_col + s, n_col)
            arrived(y_in.at[k], y_recv.at[k])

        each(n_col, wait_y)
        y_in[me_col] = y_ref[pl.ds(pl.multiple_of(me_col * y_lines, 8), y_lines), :]
        y_total = y_in[0]
        for k in range(1, n_col):
            y_total = y_total + y_in[k]
        y_own_ref[...] = y_total

    eye = (
        lax.broadcasted_iota(jnp.int32, (BLK, BLK), 0) == lax.broadcasted_iota(jnp.int32, (BLK, BLK), 1)
    ).astype(jnp.float32)
    slab = rows // (BLK // SUB)

    def solve_slab(i, s):
        lines = pl.ds(pl.multiple_of(s * slab, 8), slab)
        hi = (i + 1) * BLK
        part = turned_dot(matrix_ref[lines, :hi], w_ref[i, :, :hi])
        if i * BLK >= NB:
            line = me_row * rows + s * slab + lax.broadcasted_iota(jnp.int32, (slab, BLK), 0)
            part = jnp.where(line >= i * BLK // NB * NB, part, 0.0)
        solved_ref[i, lines, :] = part

    def beside(i, s):
        if i == 0:
            z_slab(s)
        else:
            solve_slab(i - 1, s)
        if i == 1:
            y_slab(s, order)

    @pl.when(on_panel)
    def _():
        for i in range(blocks):
            lo, hi = i * BLK, (i + 1) * BLK
            arrived(pieces_of(i, n_row - 1), d_recv.at[i])
            if i == 1:
                each(n_row, lambda s: z_copy(s).start())
            own_row = m_ref[i, :, lo:]
            if i:
                left = jnp.concatenate([m_ref[b, :, lo:hi].T for b in range(i)], axis=1)
                own_row = own_row - plain_dot(left, m_ref[:i, :, lo:].reshape(lo, order - lo))
                w_ref[i, :, :lo] = -plain_dot(left, w_ref[:i, :, :lo].reshape(lo, lo))
            diag = own_row[:, :BLK]
            x_ref[:, :BLK] = 0.5 * (diag + diag.T)
            x_ref[:, BLK:] = eye
            if hi < order:
                m_ref[i, :, hi:] = own_row[:, BLK:]
            inverse_factor(x_ref, functools.partial(beside, i))
            if i == 1:
                each(n_col, lambda s: y_copy(s).start())
            if i > 1:
                solved_copy(i - 1).start()
            if i == 4:
                sum_z()
            w_diag = x_ref[:, BLK:]
            w_ref[i, :, lo:hi] = w_diag
            if i:
                w_ref[i, :, :lo] = plain_dot(w_diag, w_ref[i, :, :lo])
            if hi < order:
                m_ref[i, :, hi:] = plain_dot(w_diag, m_ref[i, :, hi:])
                w_ref[i, :, hi:] = jnp.zeros((BLK, order - hi), jnp.float32)
            if i == 4:
                each(n_row, lambda s: z_all_copy(s).start())

        def last(s, carry):
            solve_slab(blocks - 1, s)
            return carry

        lax.fori_loop(0, BLK // SUB, last, 0)

    sum_y()

    @pl.when(on_panel)
    def _():
        solved_copy(blocks - 1).start()
        panel_ref[...] = solved_ref[0]

        def wait_all(s):
            k = lax.rem(me_row + s, n_row)
            lines = z_all_ref.at[pl.ds(pl.multiple_of(k * z_lines, 8), z_lines)]
            arrived(lines, zall_recv.at[k])

        each(n_row, wait_all)
        inverse = w_ref[...].reshape(order, order)
        pair = 2 * BLK
        weights = jnp.concatenate(
            [
                turned_dot(z_all_ref[:, : p + pair], inverse[p : p + pair, : p + pair])
                for p in range(0, order, pair)
            ],
            axis=1,
        )
        wide = jnp.concatenate([solved_ref[i] for i in range(blocks)], axis=1)
        half = fix_ref.shape[0] // 2
        for part in (1, 0):
            lines = slice(part * half, (part + 1) * half)
            fix_ref[lines, :] = turned_dot(weights[lines, :], wide)
            for to in range(part * n_col // 2, (part + 1) * n_col // 2):
                if to:
                    fix_copy(to).start()
        share_ref[...] = fix_ref[0:y_lines, :]
        each(n_row, lambda s: z_copy(s).wait_send())
        each(n_row, lambda s: z_all_copy(s).wait_send())
        each(n_col, lambda s: solved_copy(s).wait_send())
        for to in range(1, n_col):
            fix_copy(to).wait_send()
        for b in range(blocks):
            arrived(pieces_of(b, n_row - 1), next_send.at[b])

    @pl.when(me_col != 0)
    def _():
        arrived(panel_ref, s_recv.at[0])
        arrived(share_ref, fix_recv.at[0])

    each(n_col, lambda s: y_copy(s).wait_send())
    for root in range(n_roots):
        @pl.when(on_panel & (me_row == root))
        def _(root=root):
            for b, first, last in sent[root]:
                count = last - first - (first <= root < last)
                arrived(pieces_of(b, count), first_send.at[b])


def panel_parts(matrix, probe, probe_rows, order, n_row, n_col):
    rows, columns = matrix.shape[0], probe.shape[1]
    lines_z, lines_y = columns // n_row, columns // n_col
    width = order // n_col
    dma = pltpu.SemaphoreType.DMA
    whole = functools.partial(jax.ShapeDtypeStruct, dtype=jnp.float32)
    return pl.pallas_call(
        panel_kernel,
        out_shape=(
            whole((rows, width)),
            whole((lines_y, rows)),
            whole((lines_y, rows)),
        ),
        in_specs=[pl.BlockSpec(memory_space=pltpu.VMEM)] * 3,
        out_specs=[pl.BlockSpec(memory_space=pltpu.VMEM)] * 3,
        scratch_shapes=[
            pltpu.VMEM((columns, order), jnp.float32),
            pltpu.VMEM((columns, rows), jnp.float32),
            pltpu.VMEM((order // BLK, BLK, order), jnp.float32),
            pltpu.VMEM((n_col, rows, width), jnp.float32),
            pltpu.VMEM((columns, order), jnp.float32),
            pltpu.VMEM((columns, rows), jnp.float32),
            pltpu.VMEM((order // BLK, BLK, order), jnp.float32),
            pltpu.VMEM((order // BLK, BLK // n_row, order), jnp.float32),
            pltpu.VMEM((BLK, 2 * BLK), jnp.float32),
            pltpu.VMEM((n_row, lines_z, order), jnp.float32),
            pltpu.VMEM((n_col, lines_y, rows), jnp.float32),
            *[dma((order // BLK,))] * 4,
            *[dma((n_row,))] * 4,
            *[dma((n_col,))] * 3, dma((1,)), dma((n_col,)), dma((1,)),
        ],
        compiler_params=pltpu.CompilerParams(has_side_effects=True, vmem_limit_bytes=60 << 20),
        cost_estimate=pl.CostEstimate(flops=3_000_000_000, bytes_accessed=16 << 20, transcendentals=0),
        name="panel_parts",
    )(matrix, probe, probe_rows)


def per_device(front, child_tiles, tile_target, tile_count, probe):
    n_row, n_col = lax.axis_size("row"), lax.axis_size("col")
    devices = n_row * n_col
    me_row, me_col = lax.axis_index("row"), lax.axis_index("col")
    rows, cols = front.shape
    tile_rows, tile_cols = rows // TB, cols // TB
    grid = tile_cols * n_col
    held = child_tiles.shape[0]
    start = PANELS * NB
    slot_index = jnp.arange(held, dtype=jnp.int32)
    live = slot_index % SLOTS < tile_count[slot_index // SLOTS]
    first_row, first_col = tile_target // grid, tile_target % grid
    target_row = jnp.concatenate([first_row, first_col])
    target_col = jnp.concatenate([first_col, first_row])
    owner = target_row // tile_rows * n_col + target_col // tile_cols
    in_row, in_col = target_row % tile_rows, target_col % tile_cols
    upright = jnp.arange(2 * held) < held
    upright_code = 2 * (in_col // 2 * tile_rows + in_row) + in_col % 2
    blocks = cols // LANES * tile_rows
    flips = -(-rows // LANES) * tile_cols
    turned_code = 2 * (blocks + in_row // 2 * tile_cols + in_col) + in_row % 2
    code = jnp.where(upright, upright_code, turned_code)
    code = jnp.where(jnp.concatenate([live, live]), code, 2 * (blocks + flips))
    order = jnp.arange(2 * held, dtype=jnp.int32)
    same = (owner[:, None] == owner[None, :]) & (order[None, :] < order[:, None])
    slot = 2 * owner + jnp.sum(same.astype(jnp.int32), axis=1)
    at_slot = slot[None, :] == order[:, None]
    source = jnp.sum(jnp.where(at_slot, (order % held)[None, :], 0), axis=1)
    sent_code = jnp.sum(jnp.where(at_slot, code[None, :], 0), axis=1)
    outgoing = packed(child_tiles, source)
    chunks = outgoing.shape[1]
    code_lines = jnp.pad(sent_code.reshape(devices, 1, 2), ((0, 0), (0, 0), (0, LANES - 2)))
    incoming, landing, probe_rows = exchanged(
        outgoing.reshape(devices, 2 * chunks, LANES), code_lines, probe, rows
    )
    matrix = placed(front, incoming.reshape(2 * devices, chunks, LANES), landing[:, 0, :2].reshape(-1))

    global_rows = me_row * rows + jnp.arange(rows, dtype=jnp.int32)
    panel_factor, y_own, fix_own = panel_parts(matrix, probe, probe_rows, start, n_row, n_col)
    sketch = jnp.where((global_rows >= start)[:, None], (y_own - fix_own).T, 0.0)
    return (panel_factor, sketch)


def solution(mesh):
    return jax.shard_map(
        per_device,
        mesh=mesh,
        in_specs=(
            P("row", "col"),
            P(("row", "col"), None),
            P(("row", "col")),
            P(("row", "col")),
            P("col", None),
        ),
        out_specs=(P("row", "col"), P("row", "col")),
        check_vma=False,
    )
```
